32 devices in a mesh: dp: 8 (over y, x, core), tp: 4 (over z).
Axes of the slice: x: 2, y: 2, z: 4, core: 2. Of those that a mesh axis runs over, the one named last changes fastest.
Arguments:
- inputs: bfloat16 [8, 768, 1280], P('dp', 'tp'), may hold values from -6 to 6
- saved_hidden: bfloat16 [8, 768, 5120], P('dp', None, 'tp'), may hold values from -8 to 8
- upstream: bfloat16 [8, 768, 1280], P('dp', 'tp'), may hold values from -6 to 6
- w_in: bfloat16 [1280, 5120], P(None, 'tp'), may hold values from -0.15625 to 0.15625
- w_out: bfloat16 [5120, 1280], P('tp'), may hold values from -0.078125 to 0.078125
- kernel: float32 [7, 1280], replicated, may hold values from -2 to 2
Outputs:
- grad_inputs: bfloat16 [8, 768, 1280], P('dp', 'tp')
- grad_w_in: float32 [1280, 5120], P(None, 'tp')
- grad_w_out: float32 [5120, 1280], P('tp')
- grad_bias: float32 [5120], P('tp')
- grad_kernel: float32 [7, 1280], replicated
The draws below stay inside these ranges and needn't reach their ends.
All inputs are finite; a program needn't handle non-finite values.
Results may differ from the reference program's by a relative error of at most 0.02.
Values may be sent and summed in bfloat16 or wider, within the bound.
A program may use at most 128 MiB of HBM per device.

```python
from functools import partial
import jax
import jax.numpy as jnp
from jax import lax

D = 1280
FF = 5120
KW = 7
SEQ = 768
SEQS = 8
N_TP = 4


def shard_levels(stream_key, dims, pieces, low, top_value):
    gain = 1.0
    for position, blocks in pieces:
        draws = jax.random.uniform(jax.random.fold_in(jax.random.fold_in(stream_key, 6), position), (blocks,), jnp.float32, low / len(pieces), top_value / len(pieces))
        gain = gain * jnp.repeat(jnp.exp(draws), dims[position] // blocks).reshape((-1,) + (1,) * (len(dims) - 1 - position))
    return gain


def normal_values(rng, dims, width, reach, split=(), dtype=jnp.bfloat16):
    values = width * jax.random.normal(rng, dims, jnp.float32)
    if split:
        values = values * shard_levels(rng, dims, split, -0.22, 0.18)
    return jnp.clip(values, -reach, reach).astype(dtype)


def setup_inputs(seed: int = 0) -> dict:
    key_of = jax.random.split(jax.random.key(seed), 7)
    return {
        "inputs": normal_values(key_of[0], (SEQS, SEQ, D), 1.0, 6.0, ((0, 8), (1, 4))),
        "saved_hidden": normal_values(key_of[1], (SEQS, SEQ, FF), 1.5, 8.0, ((0, 8), (2, 4))),
        "upstream": normal_values(key_of[2], (SEQS, SEQ, D), 1.0, 6.0, ((0, 8), (1, 4))),
        "w_in": normal_values(key_of[3], (D, FF), D ** -0.5, 0.15625, ((1, 4),)),
        "w_out": normal_values(key_of[4], (FF, D), FF ** -0.5, 0.078125, ((0, 4),)),
        "kernel": normal_values(key_of[5], (KW, D), 0.3, 2.0, (), jnp.float32),
    }


def gelu_exact(value):
    return jax.nn.gelu(value, approximate=False)

def one_sequence(carry, items, w_in, w_out, kernel):
    total_in, total_out, total_bias, total_kernel = carry
    inputs, hidden, upstream = items
    length = inputs.shape[0]
    inputs_f = inputs.astype(jnp.float32)
    padded = jnp.pad(inputs_f, ((3, 3), (0, 0)))
    mixed = inputs_f
    for tap in range(KW):
        mixed = mixed + kernel[tap] * padded[tap:tap + length]
    mixed = mixed.astype(jnp.bfloat16)
    hidden_f = hidden.astype(jnp.float32)
    activated = gelu_exact(hidden_f).astype(jnp.bfloat16)
    back_hidden = jnp.dot(upstream, w_out.T, preferred_element_type=jnp.float32)
    grad_hidden = jax.vjp(gelu_exact, hidden_f)[1](back_hidden)[0].astype(jnp.bfloat16)
    total_out = total_out + jnp.dot(activated.T, upstream, preferred_element_type=jnp.float32)
    total_in = total_in + jnp.dot(mixed.T, grad_hidden, preferred_element_type=jnp.float32)
    total_bias = total_bias + lax.optimization_barrier(jnp.sum(grad_hidden.astype(jnp.float32), axis=0))
    block = FF // N_TP
    hidden_blocks = grad_hidden.reshape(length, N_TP, block).astype(jnp.float32)
    weight_blocks = w_in.reshape(D, N_TP, block).astype(jnp.float32)
    parts = jnp.einsum('lnf,dnf->nld', hidden_blocks, weight_blocks).astype(jnp.bfloat16)
    parts = lax.optimization_barrier(parts).astype(jnp.float32)
    grad_mixed = (upstream.astype(jnp.float32) + lax.optimization_barrier(jnp.sum(parts, axis=0))).astype(jnp.bfloat16)
    grad_f = grad_mixed.astype(jnp.float32)
    grad_pad = jnp.pad(grad_f, ((3, 3), (0, 0)))
    grad_inputs = grad_f
    taps = []
    for tap in range(KW):
        grad_inputs = grad_inputs + kernel[tap] * grad_pad[6 - tap:6 - tap + length]
        taps.append(lax.optimization_barrier(jnp.sum(grad_f * padded[tap:tap + length], axis=0)))
    total_kernel = total_kernel + jnp.stack(taps)
    return ((total_in, total_out, total_bias, total_kernel), grad_inputs.astype(jnp.bfloat16))

def reference(inputs, saved_hidden, upstream, w_in, w_out, kernel):
    start = (jnp.zeros((D, FF), jnp.float32), jnp.zeros((FF, D), jnp.float32), jnp.zeros((FF,), jnp.float32), jnp.zeros((KW, D), jnp.float32))
    step = partial(one_sequence, w_in=w_in, w_out=w_out, kernel=kernel)
    totals, grad_inputs = lax.scan(step, start, (inputs, saved_hidden, upstream))
    return (grad_inputs, totals[0], totals[1], totals[2], totals[3])
```

```python
import functools

import jax
import jax.numpy as jnp
from jax import lax
from jax.experimental import pallas as pl
from jax.experimental.pallas import tpu as pltpu
from jax.sharding import PartitionSpec as P

KW = 7
EDGE = 16
ROWS = 768
FAR = 10
LOOK = 2
VMEM = 45 * 2**20
UP_SHARES = (1,) * 5
MIX_SHARES = (1,) * 5
SUM_SHARES = (1,) * 5
F32 = jnp.float32
BF16 = jnp.bfloat16
MESH = pl.DeviceIdType.MESH


def dot(a, b, dims):
    return lax.dot_general(a, b, (dims, ((), ())), preferred_element_type=F32)


def chunk_of(size):
    return 256 if size % 256 == 0 else size


def scoped(function):
    def wrapped(*args):
        with jax.named_scope(function.__name__ + "".join(f"_{a}" for a in args if isinstance(a, int))):
            return function(*args)

    return wrapped


def cuts(width, unit, shares):
    if width % unit or width // unit < len(shares):
        return [width]
    units = width // unit
    total = sum(shares)
    edges = [units * sum(shares[:i]) // total for i in range(len(shares) + 1)]
    return [(b - a) * unit for a, b in zip(edges, edges[1:])]


def body(
    n, dp_size, up_wide, mix_wide, sum_wide, rows_of,
    x_hbm, h_hbm, up_hbm, win_hbm, wout_hbm, k_ref, gin_ref, gk_ref, gb_ref, *refs,
):
    def take(count):
        nonlocal refs
        got, refs = refs[:count], refs[count:]
        return got

    up_parts, mix_parts, sum_parts = len(up_wide), len(mix_wide), len(sum_wide)
    parts = up_parts + mix_parts
    finals = take(parts)
    accs = take(parts)
    psends = take(parts)
    precvs = take(parts)
    rsends = take(parts)
    rrecvs = take(parts)
    gathers = take(parts)
    sums = take(sum_parts)
    zrecvs = take(sum_parts)
    (
        h_ref, win_ref, wout_ref, act, gh, xpad, gpad, bias, kb, kp, k1, k2, k3,
        ls, hl, ul, hs, hr, us, uf, ur, zs, zr, ps, pr, rs, rr, ds, dr, gs, gr,
        kbs, kbr, kps, kpr, k1s, k1r, k2s, k2r, k3s, k3r,
    ) = refs
    chips = dp_size // 2
    me = lax.axis_index("tp")
    dp = lax.axis_index("dp")
    core = lax.rem(dp, 2)
    chip = dp // 2
    tokens, width = x_hbm.shape
    total_rows, hidden = h_ref.shape
    up_at = [sum(up_wide[:i]) for i in range(up_parts)]
    mix_at = [sum(mix_wide[:i]) for i in range(mix_parts)]
    sum_at = [sum(sum_wide[:i]) for i in range(sum_parts)]
    tall = chunk_of(hidden)
    bits = chips.bit_length() - 1

    def mirror(i):
        return sum((i // 2**p) % 2 * 2 ** (bits - 1 - p) for p in range(bits))

    spots = (chip, mirror(chip))
    halves = [chips >> (s + 1) for s in range(bits)]
    starts = [sum(halves[:s]) for s in range(bits)]

    def span(d, s, other):
        h = halves[s]
        side = lax.rem(spots[d] // h, 2)
        low = spots[d] // h * h
        return low + (h - 2 * h * side if other else 0)

    def peer(d, s):
        h = halves[s]
        spot = spots[d] + h - 2 * h * lax.rem(spots[d] // h, 2)
        return (mirror(spot) if d else spot) * 2 + core

    partner = dp + 1 - 2 * core

    barrier = pltpu.get_barrier_semaphore()
    for j in range(1, n):
        pl.semaphore_signal(
            barrier, inc=1, device_id=(dp, lax.rem(me + j, n)), device_id_type=MESH
        )
    for j in range(1, dp_size):
        pl.semaphore_signal(
            barrier, inc=1, device_id=(lax.rem(dp + j, dp_size), me), device_id_type=MESH
        )
    pl.semaphore_wait(barrier, n - 1 + dp_size - 1)

    def send(src, dst, s, r, to):
        return pltpu.make_async_remote_copy(
            src_ref=src, dst_ref=dst, send_sem=s, recv_sem=r, device_id=to, device_id_type=MESH
        )

    pending = []

    def start(cond, make):
        if cond is None:
            make().start()
        else:

            @pl.when(cond)
            def _():
                make().start()

        pending.append((cond, make))

    ways = (0, 1)
    step_of = (1, -1)
    room = (me, n - 1 - me)
    ahead = (n - 1 - me, me)

    def block_rows(b):
        return pl.ds(pl.multiple_of(b * tokens, tokens), tokens)

    loads = [
        pltpu.make_async_copy(x_hbm, xpad.at[pl.ds(EDGE, tokens)], ls.at[0]),
        pltpu.make_async_copy(wout_hbm, wout_ref, ls.at[1]),
        pltpu.make_async_copy(win_hbm, win_ref, ls.at[2]),
    ]

    def load_hidden(b):
        at = pl.ds(b * tokens, tokens)
        return pltpu.make_async_copy(h_hbm.at[at], h_ref.at[at], hl.at[b])

    def load_up(c):
        src = up_hbm.at[:, pl.ds(up_at[c], up_wide[c])]
        return pltpu.make_async_copy(src, gathers[c].at[block_rows(me)], ul.at[c])

    def place(k, b):
        return gathers[k].at[block_rows(b)]

    def source(k, b, own):
        if own and k < up_parts:
            return up_hbm.at[:, pl.ds(up_at[k], up_wide[k])]
        return place(k, b)

    def chain(k, d, back):
        b = jnp.clip(me - step_of[d] * back, 0, n - 1)
        to = (dp, jnp.clip(me + step_of[d], 0, n - 1))
        return send(source(k, b, back == 0), place(k, b), us.at[k, d, b], ur.at[k, d, b], to)

    def far(k, d):
        to = (dp, jnp.clip(me + 2 * step_of[d], 0, n - 1))
        return send(source(k, me, True), place(k, me), uf.at[k, d], ur.at[k, d, me], to)

    def far_used(k):
        return k < FAR

    def own_send(k, d, cond):
        start(cond & (ahead[d] > 0), functools.partial(chain, k, d, 0))
        if far_used(k):
            start(cond & (room[d] == 0) & (ahead[d] > 1), functools.partial(far, k, d))

    def x_edge(d):
        to = (dp, jnp.clip(me + step_of[d], 0, n - 1))
        src = x_hbm.at[pl.ds(tokens - EDGE if d == 0 else 0, EDGE)]
        dst = xpad.at[pl.ds(0 if d == 0 else EDGE + tokens, EDGE)]
        return send(src, dst, hs.at[d], hr.at[d], to)

    for d in ways:
        start(ahead[d] > 0, functools.partial(x_edge, d))
    for k in range(LOOK):
        for d in ways:
            own_send(k, d, me >= 0)
    for k in range(LOOK, up_parts):
        for d in ways:
            own_send(k, d, room[d] == 0)
    load_hidden(0).start()
    loads[0].start()
    for j in range(1, n):
        load_hidden(j).start()
    for c in range(up_parts):
        load_up(c).start()
    for load in loads[1:]:
        load.start()

    if act.shape[1] > hidden:
        act[:, pl.ds(hidden, act.shape[1] - hidden)] = jnp.zeros(
            (total_rows, act.shape[1] - hidden), BF16
        )
    bias[...] = jnp.zeros_like(bias)

    @pl.when(me == 0)
    def _():
        xpad[pl.ds(0, EDGE), :] = jnp.zeros((EDGE, width), BF16)
        gpad[pl.ds(0, EDGE), :] = jnp.zeros((EDGE, width), BF16)

    @pl.when(me == n - 1)
    def _():
        xpad[pl.ds(EDGE + tokens, EDGE), :] = jnp.zeros((EDGE, width), BF16)
        gpad[pl.ds(EDGE + tokens, EDGE), :] = jnp.zeros((EDGE, width), BF16)

    @scoped
    def gelu(b):
        load_hidden(b).wait()

        def gelu_step(i, _):
            at = pl.ds(pl.multiple_of(b * tokens + i * 32, 32), 32)
            v = h_ref[at, :].astype(F32)
            cdf = 0.5 + 0.5 * lax.erf(v * 0.7071067811865476)
            act[at, pl.ds(0, hidden)] = (v * cdf).astype(BF16)
            gh[at, :] = (cdf + v * (0.3989422804014327 * jnp.exp(-0.5 * v * v))).astype(BF16)
            return 0

        lax.fori_loop(0, tokens // 32, gelu_step, 0)

    @scoped
    def mix():
        for c in range(mix_parts):

            def mix_step(i, _, c=c):
                lane = pl.ds(pl.multiple_of(i * 128, 128), 128)
                at = pl.ds(pl.multiple_of(mix_at[c] + i * 128, 128), 128)
                x = xpad[:, at].astype(F32)
                taps = k_ref[:, at]
                total = x[EDGE : EDGE + tokens]
                for tap in range(KW):
                    low = EDGE - 3 + tap
                    total = total + taps[tap : tap + 1] * x[low : low + tokens]
                gathers[up_parts + c][block_rows(me), lane] = total.astype(BF16)
                return 0

            lax.fori_loop(0, mix_wide[c] // 128, mix_step, 0)

    @scoped
    def grad_dot(w):
        if w < up_parts:
            left, right = act, gathers[w]
        else:
            left, right = gathers[w], gh
        high = 2 * chips * rows_of[w]
        for half in (1 - core, core):
            lane = pl.ds(pl.multiple_of(half * high, 128), high)
            value = dot(left[:, lane], right[...], ((0,), (0,)))
            if half is core:
                accs[w][...] = value
            else:
                psends[w][...] = value.astype(BF16)
                start(None, functools.partial(pair_copy, w))

    group = tokens * max(g for g in range(1, n + 1) if n % g == 0 and tokens * g <= ROWS)

    @scoped
    def back_dot():
        def back_step(i, _):
            at = pl.ds(pl.multiple_of(i * tall, tall), tall) if tall < hidden else pl.ds(0, hidden)

            def group_step(g, _):
                row = pl.ds(pl.multiple_of(g * group, group), group)
                back = None
                for c in range(up_parts):
                    term = dot(
                        gathers[c][row, :], wout_ref[at, pl.ds(up_at[c], up_wide[c])], ((1,), (1,))
                    )
                    back = term if back is None else back + term
                grad = (gh[row, at].astype(F32) * back).astype(BF16)
                gh[row, at] = grad
                bias[:, at] += jnp.sum(grad.astype(F32), axis=0, keepdims=True)
                return 0

            if group == total_rows:
                group_step(0, 0)
            else:
                lax.fori_loop(0, total_rows // group, group_step, 0)
            return 0

        lax.fori_loop(0, hidden // tall, back_step, 0)

    @scoped
    def part_dot(r):
        wide = chunk_of(sum_wide[r])

        def part_step(i, _):
            lane = pl.ds(pl.multiple_of(i * wide, wide), wide)
            at = pl.ds(pl.multiple_of(sum_at[r] + i * wide, wide), wide)

            def group_step(g, _):
                row = pl.ds(pl.multiple_of(g * group, group), group)
                sums[r][row, lane] = dot(gh[row, :], win_ref[at, :], ((1,), (1,))).astype(BF16)
                return 0

            if group == total_rows:
                group_step(0, 0)
            else:
                lax.fori_loop(0, total_rows // group, group_step, 0)
            return 0

        lax.fori_loop(0, sum_wide[r] // wide, part_step, 0)

    def rows_at(w, d, block):
        return pl.ds(pl.multiple_of((d * chips + block) * rows_of[w], 8), rows_of[w])

    def pair_copy(w):
        return send(psends[w], precvs[w], ps.at[w], pr.at[w], (partner, me))

    def own(w, d, block):
        at = rows_at(w, d, block)
        return accs[w][at, :] + precvs[w][at, :].astype(F32)

    def ring_reduce(w, d, s):
        at = pl.ds(starts[s], halves[s])
        return send(
            rsends[w].at[d, at], rrecvs[w].at[d, at], rs.at[w, d, s], rr.at[w, d, s],
            (peer(d, s), me),
        )

    def ring_gather(w, d, s, other):
        ref = finals[w].at[core, d, pl.ds(span(d, s, other), halves[s])]
        at = 2 * bits - 1 - s
        return send(ref, ref, rs.at[w, d, at], rr.at[w, d, at], (peer(d, s), me))

    def across(w, d, s, half):
        if s == bits:
            ref = finals[w].at[half, d, pl.ds(spots[d], 1)]
        else:
            ref = finals[w].at[half, d, pl.ds(span(d, s, True), halves[s])]
        return send(ref, ref, ds.at[w, d, s], dr.at[w, d, s], (partner, me))

    last = 2 * bits

    @scoped
    def ring_step(w, s):
        acc, rsend, rrecv, final = accs[w], rsends[w], rrecvs[w], finals[w]
        if s == 0:
            pair_copy(w).wait_recv()
        for d in ways:
            if s <= bits:
                if s > 0:
                    ring_reduce(w, d, s - 1).wait_recv()

                def value(block, s=s, d=d):
                    if s == 0:
                        return own(w, d, block)
                    got = rrecv[d, starts[s - 1] + block - span(d, s - 1, False)].astype(F32)
                    if s == 1:
                        return own(w, d, block) + got
                    return acc[rows_at(w, d, block), :] + got

                if s == bits:
                    final[core, d, spots[d]] = value(spots[d]).astype(BF16)
                    start(None, functools.partial(ring_gather, w, d, s - 1, False))
                    start(None, functools.partial(across, w, d, bits, core))
                    continue
                for j in range(halves[s]):
                    rsend[d, starts[s] + j] = value(span(d, s, True) + j).astype(BF16)
                start(None, functools.partial(ring_reduce, w, d, s))
                if s > 0:
                    for j in range(halves[s]):
                        block = span(d, s, False) + j
                        acc[rows_at(w, d, block), :] = value(block)
            else:
                step = 2 * bits - s
                ring_gather(w, d, step, True).wait_recv()
                if step > 0:
                    start(None, functools.partial(ring_gather, w, d, step - 1, False))
                start(None, functools.partial(across, w, d, step, core))

    @scoped
    def ring_end(w):
        for d in ways:
            for s in range(bits + 1):
                across(w, d, s, 1 - core).wait_recv()

    def target(d, t, behind):
        place = room[d] - behind
        block = n - 1 - t + place
        return block if d == 0 else n - 1 - block

    def z_slot(d, block, owner):
        return jnp.where((block == owner) & (d == 1), n, block)

    def z_send(r, d, t):
        block = jnp.clip(target(d, t, 0), 0, n - 1)
        to = jnp.clip(me + step_of[d], 0, n - 1)
        return send(
            sums[r].at[block_rows(block)], zrecvs[r].at[z_slot(d, block, to)],
            zs.at[r, d, t], zr.at[r, d, t], (dp, to),
        )

    def z_arrive(r, d, t):
        block = jnp.clip(target(d, t, 1), 0, n - 1)
        slot = zrecvs[r].at[z_slot(d, block, me)]
        return send(slot, slot, zs.at[r, d, t], zr.at[r, d, t], (dp, jnp.clip(me + 1, 0, n - 1)))

    @scoped
    def z_step(r, t):
        for d in ways:
            if t > 0:

                @pl.when((room[d] >= 1) & (room[d] - 1 <= t - 1))
                def _(d=d):
                    z_arrive(r, d, t - 1).wait_recv()
                    if t < n - 1:
                        block = jnp.clip(target(d, t - 1, 1), 0, n - 1)
                        at = block_rows(block)
                        sums[r][at, :] = (
                            sums[r][at, :].astype(F32) + zrecvs[r][z_slot(d, block, me)].astype(F32)
                        ).astype(BF16)

            if t < n - 1:
                start(
                    (room[d] <= t) & (room[d] > 0) & (ahead[d] > 0),
                    functools.partial(z_send, r, d, t),
                )

    def z_first(r):
        for t in range(n - 1):
            for d in ways:
                start((room[d] == 0) & (ahead[d] > 0), functools.partial(z_send, r, d, t))

    active = []

    def tick(count=1):
        for _ in range(count):
            for item in list(active):
                ring_step(item[0], item[1])
                item[1] += 1
                if item[1] > last:
                    active.remove(item)

    def relays(k, d, back):
        go = (room[d] >= back) & (ahead[d] > 0)
        return go & (room[d] > 1) if far_used(k) and back == 1 else go

    @scoped
    def forward(k):
        for back in range(1, n):
            for d in ways:
                if back < n - 1:

                    @pl.when(relays(k, d, back))
                    def _(d=d):
                        chain(k, d, back).wait_recv()

                    start(relays(k, d, back), functools.partial(chain, k, d, back))
                if k + LOOK < parts:
                    own_send(k + LOOK, d, room[d] == back)

    @scoped
    def arrive(k):
        for back in range(1, n):
            for d in ways:

                @pl.when((room[d] >= back) & jnp.logical_not(relays(k, d, back)))
                def _(d=d):
                    chain(k, d, back).wait_recv()

    gelu(0)
    loads[0].wait()
    for d in ways:

        @pl.when(room[d] > 0)
        def _(d=d):
            x_edge(d).wait_recv()

    mix()
    for k in range(up_parts, parts):
        for d in ways:
            own_send(k, d, room[d] == 0)
    for b in range(1, n):
        gelu(b)
    for c in range(up_parts):
        load_up(c).wait()

    def bias_send(j):
        to = lax.rem(dp + j, dp_size)
        return send(kb.at[dp], kb.at[dp], kbs.at[j], kbr.at[dp], (to, me))

    def bias_arrive(j):
        src = lax.rem(dp + j, dp_size)
        return send(kb.at[src], kb.at[src], kbs.at[j], kbr.at[src], (src, me))

    sent = 0

    def relay_to(k):
        nonlocal sent
        while sent < min(k, parts):
            forward(sent)
            sent += 1

    def grad(k):
        arrive(k)
        grad_dot(k)
        tick()
        active.append([k, 1])
        ring_step(k, 0)

    for k in range(up_parts):
        relay_to(k + 1)
        if k == up_parts - 1:
            loads[1].wait()
            loads[2].wait()
        grad(k)
    relay_to(up_parts + 2)
    back_dot()
    kb[dp] = bias[...]
    for j in range(1, dp_size):
        start(None, functools.partial(bias_send, j))
    for r in range(sum_parts):
        part_dot(r)
        z_first(r)
    relay_to(parts)
    summed = 0
    for k in range(up_parts, parts):
        grad(k)
        while summed < sum_parts and summed < (k - up_parts):
            for t in range(1, n - 1):
                z_step(summed, t)
            summed += 1
    while summed < sum_parts:
        for t in range(1, n - 1):
            z_step(summed, t)
        summed += 1
    tick()
    for r in range(sum_parts):
        z_step(r, n - 1)

    @scoped
    def total_grad():
        edges = sorted(set(up_at + sum_at + [width]))
        for low, top in zip(edges, edges[1:]):
            c = max(i for i in range(up_parts) if up_at[i] <= low)
            r = max(i for i in range(sum_parts) if sum_at[i] <= low)

            def sum_step(i, _, low=low, c=c, r=r):
                at = pl.ds(pl.multiple_of(low + i * 128, 128), 128)
                lane = pl.ds(pl.multiple_of(low - sum_at[r] + i * 128, 128), 128)
                up_lane = pl.ds(pl.multiple_of(low - up_at[c] + i * 128, 128), 128)
                up = gathers[c][block_rows(me), up_lane].astype(F32)
                mine = sums[r][block_rows(me), lane].astype(F32)
                left = jnp.where(me > 0, zrecvs[r][me, :, lane].astype(F32), 0.0)
                right = jnp.where(me < n - 1, zrecvs[r][n, :, lane].astype(F32), 0.0)
                gpad[pl.ds(EDGE, tokens), at] = (up + (mine + left + right)).astype(BF16)
                return 0

            lax.fori_loop(0, (top - low) // 128, sum_step, 0)

    total_grad()

    def g_edge(d):
        to = (dp, jnp.clip(me + step_of[d], 0, n - 1))
        src = gpad.at[pl.ds(tokens if d == 0 else EDGE, EDGE)]
        dst = gpad.at[pl.ds(0 if d == 0 else EDGE + tokens, EDGE)]
        return send(src, dst, gs.at[d], gr.at[d], to)

    for d in ways:
        start(ahead[d] > 0, functools.partial(g_edge, d))

    @scoped
    def taps():
        def taps_step(i, _):
            at = pl.ds(pl.multiple_of(i * 128, 128), 128)
            g = gpad[pl.ds(EDGE, tokens), at].astype(F32)
            x = xpad[:, at].astype(F32)
            sums = [
                jnp.sum(g * x[EDGE - 3 + tap : EDGE - 3 + tap + tokens], axis=0, keepdims=True)
                for tap in range(KW)
            ]
            sums.append(jnp.zeros_like(sums[0]))
            kp[i // (width // 256), :, pl.ds(pl.multiple_of(lax.rem(i, width // 256) * 128, 128), 128)] = jnp.concatenate(sums, axis=0)
            return 0

        lax.fori_loop(0, width // 128, taps_step, 0)

    taps()

    def pair_taps():
        return send(kp.at[1 - core], kp.at[2], kps.at[0], kpr.at[0], (partner, me))

    start(None, pair_taps)
    tick()

    def k1_send(j):
        to = lax.rem(me + j, n)
        return send(k1.at[me], k1.at[me], k1s.at[j], k1r.at[me], (dp, to))

    def k1_arrive(j):
        src = lax.rem(me + j, n)
        return send(k1.at[src], k1.at[src], k1s.at[j], k1r.at[src], (dp, src))

    pair_taps().wait_recv()
    k1[me] = kp[core] + kp[2]
    for j in range(1, n):
        start(None, functools.partial(k1_send, j))
    for d in ways:

        @pl.when(room[d] > 0)
        def _(d=d):
            g_edge(d).wait_recv()

    @scoped
    def gin():
        def gin_step(i, _):
            at = pl.ds(pl.multiple_of(i * 128, 128), 128)
            g = gpad[:, at].astype(F32)
            taps = k_ref[:, at]
            total = g[EDGE : EDGE + tokens]
            for tap in range(KW):
                low = EDGE + 3 - tap
                total = total + taps[tap : tap + 1] * g[low : low + tokens]
            gin_ref[:, at] = total.astype(BF16)
            return 0

        lax.fori_loop(0, width // 128, gin_step, 0)

    gin()
    tick()

    @scoped
    def k1_wait():
        for j in range(1, n):
            k1_arrive(j).wait_recv()

    k1_wait()
    taps_sum = k1[0]
    for j in range(1, n):
        taps_sum = taps_sum + k1[j]
    k2[chip] = taps_sum

    def k2_send(j):
        to = lax.rem(chip + j, chips) * 2 + core
        return send(k2.at[chip], k2.at[chip], k2s.at[j], k2r.at[chip], (to, me))

    def k2_arrive(j):
        src = lax.rem(chip + j, chips)
        return send(k2.at[src], k2.at[src], k2s.at[j], k2r.at[src], (src * 2 + core, me))

    for j in range(1, chips):
        start(None, functools.partial(k2_send, j))
    tick()

    @scoped
    def k2_wait():
        for j in range(1, chips):
            k2_arrive(j).wait_recv()

    k2_wait()
    total = k2[0]
    for j in range(1, chips):
        total = total + k2[j]
    k3[core] = total

    def k3_copy(half):
        return send(k3.at[half], k3.at[half], k3s.at[0], k3r.at[0], (partner, me))

    start(None, functools.partial(k3_copy, core))
    while active:
        tick()
    for j in range(1, dp_size):
        bias_arrive(j).wait_recv()
    total = kb[0]
    for j in range(1, dp_size):
        total = total + kb[j]
    gb_ref[...] = total
    k3_copy(1 - core).wait_recv()
    for half in range(2):
        gk_ref[:, pl.ds(half * (width // 2), width // 2)] = k3[half, :KW]
    for w in range(parts):
        ring_end(w)

    @scoped
    def drain():
        for cond, make in pending:
            if cond is None:
                make().wait_send()
            else:

                @pl.when(cond)
                def _(make=make):
                    make().wait_send()

    drain()


def shards(n, dp_size, inputs, saved_hidden, upstream, w_in, w_out, kernel):
    chips = dp_size // 2
    tokens, width = inputs.shape[1:]
    hidden = w_in.shape[1]
    total_rows = n * tokens
    up_wide = cuts(width, 256, UP_SHARES)
    mix_wide = cuts(width, 64 * chips, MIX_SHARES)
    sum_wide = cuts(width, 256, SUM_SHARES)
    up_parts, mix_parts, sum_parts = len(up_wide), len(mix_wide), len(sum_wide)
    parts = up_parts + mix_parts
    rows_out = -(-hidden // (4 * chips * 8)) * 8
    high = rows_out * 4 * chips
    rows_of = [rows_out] * up_parts + [wide // (4 * chips) for wide in mix_wide]
    sizes = [(rows_out, wide) for wide in up_wide] + [
        (rows, hidden) for rows in rows_of[up_parts:]
    ]
    dma = pltpu.SemaphoreType.DMA
    bits = chips.bit_length() - 1
    vmem = pl.BlockSpec(memory_space=pltpu.VMEM)
    hbm = pl.BlockSpec(memory_space=pltpu.HBM)
    shape = jax.ShapeDtypeStruct
    grad_inputs, grad_kernel, grad_bias, *finals = pl.pallas_call(
        functools.partial(body, n, dp_size, up_wide, mix_wide, sum_wide, rows_of),
        out_shape=[shape((tokens, width), BF16), shape((KW, width), F32), shape((1, hidden), F32)]
        + [shape((2, 2, chips) + size, BF16) for size in sizes],
        in_specs=[hbm] * 5 + [vmem],
        out_specs=[vmem] * (3 + parts),
        scratch_shapes=[pltpu.VMEM((2 * chips * r, c), F32) for r, c in sizes]
        + [pltpu.VMEM((2 * chips * r, c), BF16) for r, c in sizes] * 2
        + [pltpu.VMEM((2, chips - 1) + size, BF16) for size in sizes] * 2
        + [pltpu.VMEM((total_rows, wide), BF16) for wide in up_wide + mix_wide]
        + [pltpu.VMEM((total_rows, wide), BF16) for wide in sum_wide]
        + [pltpu.VMEM((n + 1, tokens, wide), BF16) for wide in sum_wide]
        + [
            pltpu.VMEM((total_rows, hidden), BF16),
            pltpu.VMEM((width, hidden), BF16),
            pltpu.VMEM((hidden, width), BF16),
            pltpu.VMEM((total_rows, high), BF16),
            pltpu.VMEM((total_rows, hidden), BF16),
            pltpu.VMEM((tokens + 2 * EDGE, width), BF16),
            pltpu.VMEM((tokens + 2 * EDGE, width), BF16),
            pltpu.VMEM((1, hidden), F32),
            pltpu.VMEM((dp_size, 1, hidden), F32),
            pltpu.VMEM((3, 8, width // 2), F32),
            pltpu.VMEM((n, 8, width // 2), F32),
            pltpu.VMEM((chips, 8, width // 2), F32),
            pltpu.VMEM((2, 8, width // 2), F32),
            dma((3,)), dma((n,)), dma((up_parts,)),
            dma((2,)), dma((2,)),
            dma((parts, 2, n)), dma((parts, 2)), dma((parts, 2, n)),
            dma((sum_parts, 2, n)), dma((sum_parts, 2, n)),
            dma((parts,)), dma((parts,)),
            dma((parts, 2, 2 * bits)), dma((parts, 2, 2 * bits)),
            dma((parts, 2, bits + 1)), dma((parts, 2, bits + 1)),
            dma((2,)), dma((2,)),
            dma((dp_size,)), dma((dp_size,)),
            dma((1,)), dma((1,)),
            dma((n,)), dma((n,)),
            dma((chips,)), dma((chips,)),
            dma((1,)), dma((1,)),
        ],
        compiler_params=pltpu.CompilerParams(
            collective_id=0, has_side_effects=True, vmem_limit_bytes=VMEM if total_rows <= ROWS else 67043328
        ),
    )(
        inputs[0],
        saved_hidden[0],
        upstream[0],
        w_in,
        w_out,
        kernel,
    )
    outs = [f.reshape(high, wide) for f, wide in zip(finals, up_wide)]
    outs += [f.reshape(wide, hidden) for f, wide in zip(finals[up_parts:], mix_wide)]
    return tuple(
        pl.pallas_call(
            functools.partial(widen, up_wide, mix_wide),
            out_shape=[
                shape((1, tokens, width), BF16),
                shape((width, hidden), F32),
                shape((hidden, width), F32),
                shape((hidden,), F32),
                shape((KW, width), F32),
            ],
            in_specs=[vmem] * (parts + 3),
            out_specs=[hbm] * 3 + [vmem] + [hbm],
            scratch_shapes=[pltpu.VMEM((wide, hidden), F32) for wide in mix_wide]
            + [pltpu.VMEM((hidden, wide), F32) for wide in up_wide]
            + [dma((parts + 2,))],
            compiler_params=pltpu.CompilerParams(vmem_limit_bytes=24 * 2**20),
        )(*outs, grad_inputs, grad_kernel, grad_bias)
    )


def widen(up_wide, mix_wide, *refs):
    up_parts, mix_parts = len(up_wide), len(mix_wide)
    parts = up_parts + mix_parts
    finals, (gin, gk, gb), refs = refs[:parts], refs[parts : parts + 3], refs[parts + 3 :]
    gin_out, rows_out, cols_out, gb_out, gk_out, *refs = refs
    rows, cols, sem = refs[:mix_parts], refs[mix_parts:-1], refs[-1]
    copies = [
        pltpu.make_async_copy(gin, gin_out.at[0], sem.at[parts]),
        pltpu.make_async_copy(gk, gk_out, sem.at[parts + 1]),
    ]
    for copy in copies:
        copy.start()
    gb_out[...] = gb[0]

    def widen_one(source, target):
        high = target.shape[0]
        step = 64

        def widen_step(i, _):
            at = pl.ds(pl.multiple_of(i * step, step), step)
            target[at, :] = source[at, :].astype(F32)
            return 0

        lax.fori_loop(0, high // step, widen_step, 0)

    for c in range(mix_parts):
        widen_one(finals[up_parts + c], rows[c])
        at = pl.ds(sum(mix_wide[:c]), mix_wide[c])
        copies.append(pltpu.make_async_copy(rows[c], rows_out.at[at], sem.at[c]))
        copies[-1].start()
    for c in range(up_parts):
        widen_one(finals[c], cols[c])
        at = pl.ds(sum(up_wide[:c]), up_wide[c])
        copies.append(pltpu.make_async_copy(cols[c], cols_out.at[:, at], sem.at[mix_parts + c]))
        copies[-1].start()
    for copy in copies:
        copy.wait()


def solution(mesh):
    in_specs = (
        P("dp", "tp", None),
        P("dp", None, "tp"),
        P("dp", "tp", None),
        P(None, "tp"),
        P("tp", None),
        P(),
    )
    out_specs = (P("dp", "tp", None), P(None, "tp"), P("tp", None), P("tp"), P())
    return jax.shard_map(
        functools.partial(shards, mesh.shape["tp"], mesh.shape["dp"]),
        mesh=mesh,
        in_specs=in_specs,
        out_specs=out_specs,
        check_vma=False,
    )
```

```python
import functools

import jax
import jax.numpy as jnp
from jax import lax
from jax.experimental import pallas as pl
from jax.experimental.pallas import tpu as pltpu
from jax.sharding import PartitionSpec as P

KW = 7
EDGE = 16
ROWS = 768
FAR = 10
LOOK = 2
VMEM = 45 * 2**20
UP_SHARES = (1,) * 5
MIX_SHARES = (1,) * 5
SUM_SHARES = (1,) * 5
F32 = jnp.float32
BF16 = jnp.bfloat16
MESH = pl.DeviceIdType.MESH


def dot(a, b, dims):
    return lax.dot_general(a, b, (dims, ((), ())), preferred_element_type=F32)


def chunk_of(size):
    return 256 if size % 256 == 0 else size


def scoped(function):
    def wrapped(*args):
        with jax.named_scope(function.__name__ + "".join(f"_{a}" for a in args if isinstance(a, int))):
            return function(*args)

    return wrapped


def cuts(width, unit, shares):
    if width % unit or width // unit < len(shares):
        return [width]
    units = width // unit
    total = sum(shares)
    edges = [units * sum(shares[:i]) // total for i in range(len(shares) + 1)]
    return [(b - a) * unit for a, b in zip(edges, edges[1:])]


def body(
    n, dp_size, up_wide, mix_wide, sum_wide, rows_of,
    x_hbm, h_hbm, up_hbm, win_hbm, wout_hbm, k_ref, gin_ref, gk_ref, gb_ref, *refs,
):
    def take(count):
        nonlocal refs
        got, refs = refs[:count], refs[count:]
        return got

    up_parts, mix_parts, sum_parts = len(up_wide), len(mix_wide), len(sum_wide)
    parts = up_parts + mix_parts
    finals = take(parts)
    accs = take(parts)
    psends = take(parts)
    precvs = take(parts)
    rsends = take(parts)
    rrecvs = take(parts)
    gathers = take(parts)
    sums = take(sum_parts)
    zrecvs = take(sum_parts)
    (
        h_ref, win_ref, wout_ref, act, gh, xpad, gpad, bias, kb, kp, k1, k2, k3,
        ls, hl, ul, hs, hr, us, ur, zs, zr, ps, pr, rs, rr, ds, dr, gs, gr,
        kbs, kbr, kps, kpr, k1s, k1r, k2s, k2r, k3s, k3r,
    ) = refs
    chips = dp_size // 2
    me = lax.axis_index("tp")
    dp = lax.axis_index("dp")
    core = lax.rem(dp, 2)
    chip = dp // 2
    tokens, width = x_hbm.shape
    total_rows, hidden = h_ref.shape
    up_at = [sum(up_wide[:i]) for i in range(up_parts)]
    mix_at = [sum(mix_wide[:i]) for i in range(mix_parts)]
    sum_at = [sum(sum_wide[:i]) for i in range(sum_parts)]
    tall = chunk_of(hidden)
    bits = chips.bit_length() - 1

    def mirror(i):
        return sum((i // 2**p) % 2 * 2 ** (bits - 1 - p) for p in range(bits))

    spots = (chip, mirror(chip))
    halves = [chips >> (s + 1) for s in range(bits)]
    starts = [sum(halves[:s]) for s in range(bits)]

    def span(d, s, other):
        h = halves[s]
        side = lax.rem(spots[d] // h, 2)
        low = spots[d] // h * h
        return low + (h - 2 * h * side if other else 0)

    def peer(d, s):
        h = halves[s]
        spot = spots[d] + h - 2 * h * lax.rem(spots[d] // h, 2)
        return (mirror(spot) if d else spot) * 2 + core

    partner = dp + 1 - 2 * core

    barrier = pltpu.get_barrier_semaphore()
    for j in range(1, n):
        pl.semaphore_signal(
            barrier, inc=1, device_id=(dp, lax.rem(me + j, n)), device_id_type=MESH
        )
    for j in range(1, dp_size):
        pl.semaphore_signal(
            barrier, inc=1, device_id=(lax.rem(dp + j, dp_size), me), device_id_type=MESH
        )
    pl.semaphore_wait(barrier, n - 1 + dp_size - 1)

    def send(src, dst, s, r, to):
        return pltpu.make_async_remote_copy(
            src_ref=src, dst_ref=dst, send_sem=s, recv_sem=r, device_id=to, device_id_type=MESH
        )

    pending = []

    def start(cond, make, keep=True):
        if cond is None:
            make().start()
        else:

            @pl.when(cond)
            def _():
                make().start()

        if keep:
            pending.append((cond, make))

    def group(ref, s, r):
        return send(ref, ref, s, r, (partner, me))

    ways = (0, 1)
    step_of = (1, -1)
    room = (me, n - 1 - me)
    ahead = (n - 1 - me, me)

    def block_rows(b):
        return pl.ds(pl.multiple_of(b * tokens, tokens), tokens)

    loads = [
        pltpu.make_async_copy(x_hbm, xpad.at[pl.ds(EDGE, tokens)], ls.at[0]),
        pltpu.make_async_copy(wout_hbm, wout_ref, ls.at[1]),
        pltpu.make_async_copy(win_hbm, win_ref, ls.at[2]),
    ]

    def load_hidden(b):
        at = pl.ds(b * tokens, tokens)
        return pltpu.make_async_copy(h_hbm.at[at], h_ref.at[at], hl.at[b])

    def load_up(c):
        src = up_hbm.at[:, pl.ds(up_at[c], up_wide[c])]
        return pltpu.make_async_copy(src, gathers[c].at[block_rows(me)], ul.at[c])

    def place(k, b):
        return gathers[k].at[block_rows(b)]

    def source(k, b, own):
        if own and k < up_parts:
            return up_hbm.at[:, pl.ds(up_at[k], up_wide[k])]
        return place(k, b)

    def chain(k, d, back):
        b = jnp.clip(me - step_of[d] * back, 0, n - 1)
        to = (dp, jnp.clip(me + step_of[d], 0, n - 1))
        return send(source(k, b, back == 0), place(k, b), us.at[k, d], ur.at[k, b], to)

    def far(k, d):
        to = (dp, jnp.clip(me + 2 * step_of[d], 0, n - 1))
        return send(source(k, me, True), place(k, me), us.at[k, d], ur.at[k, me], to)

    def far_used(k):
        return k < FAR

    def own_send(k, d, cond):
        start(cond & (ahead[d] > 0), functools.partial(chain, k, d, 0), False)
        if far_used(k):
            start(cond & (room[d] == 0) & (ahead[d] > 1), functools.partial(far, k, d), False)

    def free(k):
        return 1 if far_used(k) else 0

    def later(k):
        if k == up_parts - 1:
            return range(up_parts, min(up_parts + LOOK, parts))
        if k + LOOK < up_parts or up_parts <= k < parts - LOOK:
            return [k + LOOK]
        return []

    def sent_of(m, k, d):
        front, behind = (n - 1 - m, m) if d == 0 else (m, n - 1 - m)
        if front == 0:
            return 0
        count = 1 + (far_used(k) and behind == 0 and front > 1)
        return count + sum(
            behind >= back and not (far_used(k) and back == 1 and behind == 1)
            for back in range(1, n - 1)
        )

    def x_edge(d):
        to = (dp, jnp.clip(me + step_of[d], 0, n - 1))
        src = x_hbm.at[pl.ds(tokens - EDGE if d == 0 else 0, EDGE)]
        dst = xpad.at[pl.ds(0 if d == 0 else EDGE + tokens, EDGE)]
        return send(src, dst, hs.at[d], hr.at[d], to)

    for d in ways:
        start(ahead[d] > 0, functools.partial(x_edge, d))
    for k in range(LOOK):
        for d in ways:
            own_send(k, d, me >= 0)
    for k in range(LOOK, up_parts):
        for d in ways:
            own_send(k, d, room[d] <= free(k))
    load_hidden(0).start()
    loads[0].start()
    for j in range(1, n):
        load_hidden(j).start()
    for c in range(up_parts):
        load_up(c).start()
    for load in loads[1:]:
        load.start()

    if act.shape[1] > hidden:
        act[:, pl.ds(hidden, act.shape[1] - hidden)] = jnp.zeros(
            (total_rows, act.shape[1] - hidden), BF16
        )
    bias[...] = jnp.zeros_like(bias)

    @pl.when(me == 0)
    def _():
        xpad[pl.ds(0, EDGE), :] = jnp.zeros((EDGE, width), BF16)
        gpad[pl.ds(0, EDGE), :] = jnp.zeros((EDGE, width), BF16)

    @pl.when(me == n - 1)
    def _():
        xpad[pl.ds(EDGE + tokens, EDGE), :] = jnp.zeros((EDGE, width), BF16)
        gpad[pl.ds(EDGE + tokens, EDGE), :] = jnp.zeros((EDGE, width), BF16)

    @scoped
    def gelu(b):
        load_hidden(b).wait()

        def gelu_step(i, _):
            at = pl.ds(pl.multiple_of(b * tokens + i * 32, 32), 32)
            v = h_ref[at, :].astype(F32)
            cdf = 0.5 + 0.5 * lax.erf(v * 0.7071067811865476)
            act[at, pl.ds(0, hidden)] = (v * cdf).astype(BF16)
            gh[at, :] = (cdf + v * (0.3989422804014327 * jnp.exp(-0.5 * v * v))).astype(BF16)
            return 0

        lax.fori_loop(0, tokens // 32, gelu_step, 0)

    @scoped
    def mix():
        for c in range(mix_parts):

            def mix_step(i, _, c=c):
                lane = pl.ds(pl.multiple_of(i * 128, 128), 128)
                at = pl.ds(pl.multiple_of(mix_at[c] + i * 128, 128), 128)
                x = xpad[:, at].astype(F32)
                taps = k_ref[:, at]
                total = x[EDGE : EDGE + tokens]
                for tap in range(KW):
                    low = EDGE - 3 + tap
                    total = total + taps[tap : tap + 1] * x[low : low + tokens]
                gathers[up_parts + c][block_rows(me), lane] = total.astype(BF16)
                return 0

            lax.fori_loop(0, mix_wide[c] // 128, mix_step, 0)

    @scoped
    def grad_dot(w):
        if w < up_parts:
            left, right = act, gathers[w]
        else:
            left, right = gathers[w], gh
        high = 2 * chips * rows_of[w]
        for half in (1 - core, core):
            lane = pl.ds(pl.multiple_of(half * high, 128), high)
            value = dot(left[:, lane], right[...], ((0,), (0,)))
            if half is core:
                accs[w][...] = value
            else:
                psends[w][...] = value.astype(BF16)
                start(None, functools.partial(pair_copy, w))

    batch = tokens * max(g for g in range(1, n + 1) if n % g == 0 and tokens * g <= ROWS)

    @scoped
    def back_dot():
        def back_step(i, _):
            at = pl.ds(pl.multiple_of(i * tall, tall), tall) if tall < hidden else pl.ds(0, hidden)

            def group_step(g, _):
                row = pl.ds(pl.multiple_of(g * batch, batch), batch)
                back = None
                for c in range(up_parts):
                    term = dot(
                        gathers[c][row, :], wout_ref[at, pl.ds(up_at[c], up_wide[c])], ((1,), (1,))
                    )
                    back = term if back is None else back + term
                grad = (gh[row, at].astype(F32) * back).astype(BF16)
                gh[row, at] = grad
                bias[:, at] += jnp.sum(grad.astype(F32), axis=0, keepdims=True)
                return 0

            if batch == total_rows:
                group_step(0, 0)
            else:
                lax.fori_loop(0, total_rows // batch, group_step, 0)
            return 0

        lax.fori_loop(0, hidden // tall, back_step, 0)

    @scoped
    def part_dot(r, count):
        at = pl.ds(sum_at[r], sum(sum_wide[r : r + count]))

        def group_step(g, _):
            row = pl.ds(pl.multiple_of(g * batch, batch), batch)
            value = dot(gh[row, :], win_ref[at, :], ((1,), (1,))).astype(BF16)
            for j in range(r, r + count):
                low = sum_at[j] - sum_at[r]
                sums[j][row, :] = value[:, low : low + sum_wide[j]]
            return 0

        if batch == total_rows:
            group_step(0, 0)
        else:
            lax.fori_loop(0, total_rows // batch, group_step, 0)

    def rows_at(w, d, block):
        return pl.ds(pl.multiple_of((d * chips + block) * rows_of[w], 8), rows_of[w])

    def pair_copy(w):
        return send(psends[w], precvs[w], ps.at[w], pr.at[w], (partner, me))

    def own(w, d, block):
        at = rows_at(w, d, block)
        return accs[w][at, :] + precvs[w][at, :].astype(F32)

    def ring_reduce(w, d, s):
        at = pl.ds(starts[s], halves[s])
        return send(
            rsends[w].at[d, at], rrecvs[w].at[d, at], rs.at[w], rr.at[w, s],
            (peer(d, s), me),
        )

    def ring_gather(w, d, s, other):
        ref = finals[w].at[core, d, pl.ds(span(d, s, other), halves[s])]
        at = 2 * bits - 1 - s
        return send(ref, ref, rs.at[w], rr.at[w, at], (peer(d, s), me))

    def across(w, d, s, half):
        if s == bits:
            ref = finals[w].at[half, d, pl.ds(spots[d], 1)]
        else:
            ref = finals[w].at[half, d, pl.ds(span(d, s, True), halves[s])]
        return send(ref, ref, ds.at[w], dr.at[w], (partner, me))

    last = 2 * bits

    @scoped
    def ring_step(w, s):
        acc, rsend, rrecv, final = accs[w], rsends[w], rrecvs[w], finals[w]
        if s == 0:
            pair_copy(w).wait_recv()
        else:
            j = s - 1 if s <= bits else 2 * bits - s
            both = rrecv.at[:, pl.ds(starts[j], halves[j])]
            group(both, rs.at[w], rr.at[w, s - 1]).wait_recv()
        for d in ways:
            if s <= bits:

                def value(block, s=s, d=d):
                    if s == 0:
                        return own(w, d, block)
                    got = rrecv[d, starts[s - 1] + block - span(d, s - 1, False)].astype(F32)
                    if s == 1:
                        return own(w, d, block) + got
                    return acc[rows_at(w, d, block), :] + got

                if s == bits:
                    final[core, d, spots[d]] = value(spots[d]).astype(BF16)
                    start(None, functools.partial(ring_gather, w, d, s - 1, False), False)
                    start(None, functools.partial(across, w, d, bits, core), False)
                    continue
                for j in range(halves[s]):
                    rsend[d, starts[s] + j] = value(span(d, s, True) + j).astype(BF16)
                start(None, functools.partial(ring_reduce, w, d, s), False)
                if s > 0:
                    for j in range(halves[s]):
                        block = span(d, s, False) + j
                        acc[rows_at(w, d, block), :] = value(block)
            else:
                step = 2 * bits - s
                if step > 0:
                    start(None, functools.partial(ring_gather, w, d, step - 1, False), False)
                start(None, functools.partial(across, w, d, step, core), False)

    @scoped
    def ring_end(w):
        group(finals[w].at[1 - core], ds.at[w], dr.at[w]).wait_recv()

    def target(d, t, behind):
        place = room[d] - behind
        block = n - 1 - t + place
        return block if d == 0 else n - 1 - block

    def z_slot(d, block, owner):
        return jnp.where((block == owner) & (d == 1), n, block)

    def z_send(r, d, t):
        block = jnp.clip(target(d, t, 0), 0, n - 1)
        to = jnp.clip(me + step_of[d], 0, n - 1)
        return send(
            sums[r].at[block_rows(block)], zrecvs[r].at[z_slot(d, block, to)],
            zs.at[r], zr.at[r, z_slot(d, block, to)], (dp, to),
        )

    def z_arrive(r, d, t):
        block = jnp.clip(target(d, t, 1), 0, n - 1)
        slot = z_slot(d, block, me)
        return group(zrecvs[r].at[slot], zs.at[r], zr.at[r, slot])

    @scoped
    def z_step(r, t):
        for d in ways:
            if t > 0:

                @pl.when((room[d] >= 1) & (room[d] - 1 <= t - 1))
                def _(d=d):
                    z_arrive(r, d, t - 1).wait_recv()
                    if t < n - 1:
                        block = jnp.clip(target(d, t - 1, 1), 0, n - 1)
                        at = block_rows(block)
                        sums[r][at, :] = (
                            sums[r][at, :].astype(F32) + zrecvs[r][z_slot(d, block, me)].astype(F32)
                        ).astype(BF16)

            if t < n - 1:
                start(
                    (room[d] <= t) & (room[d] > 0) & (ahead[d] > 0),
                    functools.partial(z_send, r, d, t),
                    False,
                )

    def z_first(r, t):
        for d in ways:
            start((room[d] == 0) & (ahead[d] > 0), functools.partial(z_send, r, d, t), False)

    active = []

    def tick(count=1):
        for _ in range(count):
            for item in list(active):
                ring_step(item[0], item[1])
                item[1] += 1
                if item[1] > last:
                    active.remove(item)

    def relays(k, d, back):
        go = (room[d] >= back) & (ahead[d] > 0)
        return go & (room[d] > 1) if far_used(k) and back == 1 else go

    @scoped
    def forward(k):
        for back in range(1, n):
            for d in ways:
                if back < n - 1:

                    @pl.when(relays(k, d, back))
                    def _(d=d):
                        chain(k, d, back).wait_recv()

                    start(relays(k, d, back), functools.partial(chain, k, d, back), False)
                for j in later(k):
                    own_send(j, d, (room[d] == back) & (room[d] > free(j)))

    @scoped
    def arrive(k):
        for back in range(1, n):
            for d in ways:

                @pl.when((room[d] >= back) & jnp.logical_not(relays(k, d, back)))
                def _(d=d):
                    chain(k, d, back).wait_recv()

    gelu(0)
    loads[0].wait()
    for d in ways:

        @pl.when(room[d] > 0)
        def _(d=d):
            x_edge(d).wait_recv()

    mix()
    for k in range(up_parts, parts):
        for d in ways:
            own_send(k, d, room[d] <= free(k))
    for b in range(1, n):
        gelu(b)
    for c in range(up_parts):
        load_up(c).wait()

    def bias_send(j):
        to = lax.rem(dp + j, dp_size)
        return send(kb.at[dp], kb.at[dp], kbs.at[0], kbr.at[0], (to, me))

    def bias_group():
        return group(kb.at[pl.ds(0, dp_size - 1)], kbs.at[0], kbr.at[0])

    sent = 0

    def relay_to(k):
        nonlocal sent
        while sent < min(k, parts):
            forward(sent)
            sent += 1

    def grad(k):
        arrive(k)
        grad_dot(k)
        tick()
        active.append([k, 1])
        ring_step(k, 0)

    for k in range(up_parts):
        relay_to(k + 1)
        if k == up_parts - 1:
            loads[1].wait()
            loads[2].wait()
        grad(k)
    relay_to(up_parts + 2)
    back_dot()
    kb[dp] = bias[...]
    for j in range(1, dp_size):
        start(None, functools.partial(bias_send, j), False)
    for r in range(0, sum_parts, 2):
        count = min(2, sum_parts - r)
        if r + 2 >= sum_parts:
            grad(up_parts)
        part_dot(r, count)
        for j in range(r, r + count):
            z_first(j, 0)
    for t in range(1, n - 1):
        for r in range(sum_parts):
            z_first(r, t)
    relay_to(parts)
    items = [(r, t) for t in range(1, n - 1) for r in range(sum_parts)]
    done = 0
    for k in range(up_parts, parts):
        if k > up_parts or sum_parts < 3:
            grad(k)
        goal = len(items) * (k - up_parts + 1) // max(1, mix_parts - 1)
        for item in items[done:goal]:
            z_step(*item)
        done = max(done, min(goal, len(items)))

    def g_edge(r, d):
        to = (dp, jnp.clip(me + step_of[d], 0, n - 1))
        lane = pl.ds(sum_at[r], sum_wide[r])
        src = gpad.at[pl.ds(tokens if d == 0 else EDGE, EDGE), lane]
        dst = gpad.at[pl.ds(0 if d == 0 else EDGE + tokens, EDGE), lane]
        return send(src, dst, gs.at[r, d], gr.at[r, d], to)

    @scoped
    def total_grad(r):
        edges = sorted({e for e in up_at + [width] if sum_at[r] < e < sum_at[r] + sum_wide[r]})
        edges = [sum_at[r]] + edges + [sum_at[r] + sum_wide[r]]
        for low, top in zip(edges, edges[1:]):
            c = max(i for i in range(up_parts) if up_at[i] <= low)

            def sum_step(i, _, low=low, c=c):
                at = pl.ds(pl.multiple_of(low + i * 128, 128), 128)
                lane = pl.ds(pl.multiple_of(low - sum_at[r] + i * 128, 128), 128)
                up_lane = pl.ds(pl.multiple_of(low - up_at[c] + i * 128, 128), 128)
                up = gathers[c][block_rows(me), up_lane].astype(F32)
                mine = sums[r][block_rows(me), lane].astype(F32)
                left = jnp.where(me > 0, zrecvs[r][me, :, lane].astype(F32), 0.0)
                right = jnp.where(me < n - 1, zrecvs[r][n, :, lane].astype(F32), 0.0)
                g = (up + (mine + left + right)).astype(BF16)
                gpad[pl.ds(EDGE, tokens), at] = g
                return 0

            lax.fori_loop(0, (top - low) // 128, sum_step, 0)
        for d in ways:
            start(ahead[d] > 0, functools.partial(g_edge, r, d))

    @scoped
    def taps(r):
        def taps_step(i, _):
            at = pl.ds(pl.multiple_of(sum_at[r] + i * 128, 128), 128)
            g = gpad[pl.ds(EDGE, tokens), at].astype(F32)
            x = xpad[:, at].astype(F32)
            totals = [
                jnp.sum(g * x[EDGE - 3 + tap : EDGE - 3 + tap + tokens], axis=0, keepdims=True)
                for tap in range(KW)
            ]
            totals.append(jnp.zeros_like(totals[0]))
            j = i + sum_at[r] // 128
            lane = pl.ds(pl.multiple_of(lax.rem(j, width // 256) * 128, 128), 128)
            kp[j // (width // 256), :, lane] = jnp.concatenate(totals, axis=0)
            return 0

        lax.fori_loop(0, sum_wide[r] // 128, taps_step, 0)

    @scoped
    def gin(r):
        for d in ways:

            @pl.when(room[d] > 0)
            def _(d=d):
                g_edge(r, d).wait_recv()

        def gin_step(i, _):
            at = pl.ds(pl.multiple_of(sum_at[r] + i * 128, 128), 128)
            g = gpad[:, at].astype(F32)
            taps = k_ref[:, at]
            total = g[EDGE : EDGE + tokens]
            for tap in range(KW):
                low = EDGE + 3 - tap
                total = total + taps[tap : tap + 1] * g[low : low + tokens]
            gin_ref[:, at] = total.astype(BF16)
            return 0

        lax.fori_loop(0, sum_wide[r] // 128, gin_step, 0)

    for r in range(sum_parts):
        z_step(r, n - 1)
        total_grad(r)
        taps(r)
        if r % 2:
            tick()

    def pair_taps():
        return send(kp.at[1 - core], kp.at[2], kps.at[0], kpr.at[0], (partner, me))

    start(None, pair_taps)
    for r in range(sum_parts - 1):
        gin(r)

    def k1_send(j):
        to = lax.rem(me + j, n)
        return send(k1.at[me], k1.at[me], k1s.at[0], k1r.at[0], (dp, to))

    def k1_group():
        return group(k1.at[pl.ds(0, n - 1)], k1s.at[0], k1r.at[0])

    pair_taps().wait_recv()
    k1[me] = kp[core] + kp[2]
    for j in range(1, n):
        start(None, functools.partial(k1_send, j), False)
    tick()
    gin(sum_parts - 1)

    @scoped
    def k1_wait():
        k1_group().wait_recv()

    k1_wait()
    taps_sum = k1[0]
    for j in range(1, n):
        taps_sum = taps_sum + k1[j]
    k2[chip] = taps_sum

    def k2_send(j):
        to = lax.rem(chip + j, chips) * 2 + core
        return send(k2.at[chip], k2.at[chip], k2s.at[0], k2r.at[0], (to, me))

    def k2_group():
        return group(k2.at[pl.ds(0, chips - 1)], k2s.at[0], k2r.at[0])

    for j in range(1, chips):
        start(None, functools.partial(k2_send, j), False)
    tick()

    @scoped
    def k2_wait():
        k2_group().wait_recv()

    k2_wait()
    total = k2[0]
    for j in range(1, chips):
        total = total + k2[j]
    k3[core] = total

    def k3_copy(half):
        return send(k3.at[half], k3.at[half], k3s.at[0], k3r.at[0], (partner, me))

    start(None, functools.partial(k3_copy, core))
    while active:
        tick()
    bias_group().wait_recv()
    total = kb[0]
    for j in range(1, dp_size):
        total = total + kb[j]
    gb_ref[...] = total
    k3_copy(1 - core).wait_recv()
    for half in range(2):
        gk_ref[:, pl.ds(half * (width // 2), width // 2)] = k3[half, :KW]
    for w in range(parts):
        ring_end(w)

    @scoped
    def drain():
        for m in range(n):

            @pl.when(me == m)
            def _(m=m):
                for k in range(parts):
                    for d in ways:
                        count = sent_of(m, k, d)
                        if count:
                            ref = gathers[k].at[pl.ds(0, count * tokens)]
                            group(ref, us.at[k, d], ur.at[k, 0]).wait_send()

        for w in range(parts):
            group(finals[w].at[:, :, pl.ds(0, chips - 1)], rs.at[w], rr.at[w, 0]).wait_send()
            group(finals[w].at[1 - core], ds.at[w], dr.at[w]).wait_send()
        for r in range(sum_parts):
            ref = sums[r].at[pl.ds(0, (n - 1) * tokens)]
            group(ref, zs.at[r], zr.at[r, 0]).wait_send()
        bias_group().wait_send()
        k1_group().wait_send()
        k2_group().wait_send()
        for cond, make in pending:
            if cond is None:
                make().wait_send()
            else:

                @pl.when(cond)
                def _(make=make):
                    make().wait_send()

    drain()


def shards(n, dp_size, inputs, saved_hidden, upstream, w_in, w_out, kernel):
    chips = dp_size // 2
    tokens, width = inputs.shape[1:]
    hidden = w_in.shape[1]
    total_rows = n * tokens
    up_wide = cuts(width, 256, UP_SHARES)
    mix_wide = cuts(width, 64 * chips, MIX_SHARES)
    sum_wide = cuts(width, 256, SUM_SHARES)
    up_parts, mix_parts, sum_parts = len(up_wide), len(mix_wide), len(sum_wide)
    parts = up_parts + mix_parts
    rows_out = -(-hidden // (4 * chips * 8)) * 8
    high = rows_out * 4 * chips
    rows_of = [rows_out] * up_parts + [wide // (4 * chips) for wide in mix_wide]
    sizes = [(rows_out, wide) for wide in up_wide] + [
        (rows, hidden) for rows in rows_of[up_parts:]
    ]
    dma = pltpu.SemaphoreType.DMA
    bits = chips.bit_length() - 1
    vmem = pl.BlockSpec(memory_space=pltpu.VMEM)
    hbm = pl.BlockSpec(memory_space=pltpu.HBM)
    shape = jax.ShapeDtypeStruct
    grad_inputs, grad_kernel, grad_bias, *finals = pl.pallas_call(
        functools.partial(body, n, dp_size, up_wide, mix_wide, sum_wide, rows_of),
        out_shape=[shape((tokens, width), BF16), shape((KW, width), F32), shape((1, hidden), F32)]
        + [shape((2, 2, chips) + size, BF16) for size in sizes],
        in_specs=[hbm] * 5 + [vmem],
        out_specs=[vmem] * (3 + parts),
        scratch_shapes=[pltpu.VMEM((2 * chips * r, c), F32) for r, c in sizes]
        + [pltpu.VMEM((2 * chips * r, c), BF16) for r, c in sizes] * 2
        + [pltpu.VMEM((2, chips - 1) + size, BF16) for size in sizes] * 2
        + [pltpu.VMEM((total_rows, wide), BF16) for wide in up_wide + mix_wide]
        + [pltpu.VMEM((total_rows, wide), BF16) for wide in sum_wide]
        + [pltpu.VMEM((n + 1, tokens, wide), BF16) for wide in sum_wide]
        + [
            pltpu.VMEM((total_rows, hidden), BF16),
            pltpu.VMEM((width, hidden), BF16),
            pltpu.VMEM((hidden, width), BF16),
            pltpu.VMEM((total_rows, high), BF16),
            pltpu.VMEM((total_rows, hidden), BF16),
            pltpu.VMEM((tokens + 2 * EDGE, width), BF16),
            pltpu.VMEM((tokens + 2 * EDGE, width), BF16),
            pltpu.VMEM((1, hidden), F32),
            pltpu.VMEM((dp_size, 1, hidden), F32),
            pltpu.VMEM((3, 8, width // 2), F32),
            pltpu.VMEM((n, 8, width // 2), F32),
            pltpu.VMEM((chips, 8, width // 2), F32),
            pltpu.VMEM((2, 8, width // 2), F32),
            dma((3,)), dma((n,)), dma((up_parts,)),
            dma((2,)), dma((2,)),
            dma((parts, 2)), dma((parts, n)),
            dma((sum_parts,)), dma((sum_parts, n + 1)),
            dma((parts,)), dma((parts,)),
            dma((parts,)), dma((parts, 2 * bits)),
            dma((parts,)), dma((parts,)),
            dma((sum_parts, 2)), dma((sum_parts, 2)),
            dma((1,)), dma((1,)),
            dma((1,)), dma((1,)),
            dma((1,)), dma((1,)),
            dma((1,)), dma((1,)),
            dma((1,)), dma((1,)),
        ],
        compiler_params=pltpu.CompilerParams(
            collective_id=0, has_side_effects=True, vmem_limit_bytes=VMEM if total_rows <= ROWS else 67043328
        ),
    )(
        inputs[0],
        saved_hidden[0],
        upstream[0],
        w_in,
        w_out,
        kernel,
    )
    outs = [f.reshape(high, wide) for f, wide in zip(finals, up_wide)]
    outs += [f.reshape(wide, hidden) for f, wide in zip(finals[up_parts:], mix_wide)]
    return tuple(
        pl.pallas_call(
            functools.partial(widen, up_wide, mix_wide),
            out_shape=[
                shape((1, tokens, width), BF16),
                shape((width, hidden), F32),
                shape((hidden, width), F32),
                shape((hidden,), F32),
                shape((KW, width), F32),
            ],
            in_specs=[vmem] * (parts + 3),
            out_specs=[hbm] * 3 + [vmem] + [hbm],
            scratch_shapes=[pltpu.VMEM((wide, hidden), F32) for wide in mix_wide]
            + [pltpu.VMEM((hidden, wide), F32) for wide in up_wide]
            + [dma((parts + 2,))],
            compiler_params=pltpu.CompilerParams(vmem_limit_bytes=24 * 2**20),
        )(*outs, grad_inputs, grad_kernel, grad_bias)
    )


def widen(up_wide, mix_wide, *refs):
    up_parts, mix_parts = len(up_wide), len(mix_wide)
    parts = up_parts + mix_parts
    finals, (gin, gk, gb), refs = refs[:parts], refs[parts : parts + 3], refs[parts + 3 :]
    gin_out, rows_out, cols_out, gb_out, gk_out, *refs = refs
    rows, cols, sem = refs[:mix_parts], refs[mix_parts:-1], refs[-1]
    copies = [
        pltpu.make_async_copy(gin, gin_out.at[0], sem.at[parts]),
        pltpu.make_async_copy(gk, gk_out, sem.at[parts + 1]),
    ]
    for copy in copies:
        copy.start()
    gb_out[...] = gb[0]

    def widen_one(source, target):
        high = target.shape[0]
        step = 64

        def widen_step(i, _):
            at = pl.ds(pl.multiple_of(i * step, step), step)
            target[at, :] = source[at, :].astype(F32)
            return 0

        lax.fori_loop(0, high // step, widen_step, 0)

    for c in range(mix_parts):
        widen_one(finals[up_parts + c], rows[c])
        at = pl.ds(sum(mix_wide[:c]), mix_wide[c])
        copies.append(pltpu.make_async_copy(rows[c], rows_out.at[at], sem.at[c]))
        copies[-1].start()
    for c in range(up_parts):
        widen_one(finals[c], cols[c])
        at = pl.ds(sum(up_wide[:c]), up_wide[c])
        copies.append(pltpu.make_async_copy(cols[c], cols_out.at[:, at], sem.at[mix_parts + c]))
        copies[-1].start()
    for copy in copies:
        copy.wait()


def solution(mesh):
    in_specs = (
        P("dp", "tp", None),
        P("dp", None, "tp"),
        P("dp", "tp", None),
        P(None, "tp"),
        P("tp", None),
        P(),
    )
    out_specs = (P("dp", "tp", None), P(None, "tp"), P("tp", None), P("tp"), P())
    return jax.shard_map(
        functools.partial(shards, mesh.shape["tp"], mesh.shape["dp"]),
        mesh=mesh,
        in_specs=in_specs,
        out_specs=out_specs,
        check_vma=False,
    )
```

```python
import functools

import jax
import jax.numpy as jnp
from jax import lax
from jax.experimental import pallas as pl
from jax.experimental.pallas import tpu as pltpu
from jax.sharding import PartitionSpec as P

KW = 7
EDGE = 16
ROWS = 768
FAR = 10
LOOK = 2
VMEM = 45 * 2**20
UP_SHARES = (1,) * 5
MIX_SHARES = (1,) * 5
SUM_SHARES = (1,) * 5
F32 = jnp.float32
BF16 = jnp.bfloat16
MESH = pl.DeviceIdType.MESH


def dot(a, b, dims):
    return lax.dot_general(a, b, (dims, ((), ())), preferred_element_type=F32)


def chunk_of(size):
    return 256 if size % 256 == 0 else size


def scoped(function):
    def wrapped(*args):
        with jax.named_scope(function.__name__ + "".join(f"_{a}" for a in args if isinstance(a, int))):
            return function(*args)

    return wrapped


def cuts(width, unit, shares):
    if width % unit or width // unit < len(shares):
        return [width]
    units = width // unit
    total = sum(shares)
    edges = [units * sum(shares[:i]) // total for i in range(len(shares) + 1)]
    return [(b - a) * unit for a, b in zip(edges, edges[1:])]


def body(
    n, dp_size, up_wide, mix_wide, sum_wide, rows_of,
    x_hbm, h_hbm, up_hbm, win_hbm, wout_hbm, k_ref, gin_ref, gk_ref, gb_ref, *refs,
):
    def take(count):
        nonlocal refs
        got, refs = refs[:count], refs[count:]
        return got

    up_parts, mix_parts, sum_parts = len(up_wide), len(mix_wide), len(sum_wide)
    parts = up_parts + mix_parts
    finals = take(parts)
    accs = take(parts)
    psends = take(parts)
    precvs = take(parts)
    rsends = take(parts)
    rrecvs = take(parts)
    gathers = take(parts)
    sums = take(sum_parts)
    zrecvs = take(sum_parts)
    (
        h_ref, win_ref, wout_ref, act, gh, xpad, gpad, bias, kb, kp, k1, k2, k3,
        ls, hl, ul, hs, hr, us, ur, zs, zr, ps, pr, rs, rr, ds, dr, gs, gr,
        kbs, kbr, kps, kpr, k1s, k1r, k2s, k2r, k3s, k3r,
    ) = refs
    chips = dp_size // 2
    me = lax.axis_index("tp")
    dp = lax.axis_index("dp")
    core = lax.rem(dp, 2)
    chip = dp // 2
    tokens, width = x_hbm.shape
    total_rows, hidden = h_ref.shape
    up_at = [sum(up_wide[:i]) for i in range(up_parts)]
    mix_at = [sum(mix_wide[:i]) for i in range(mix_parts)]
    sum_at = [sum(sum_wide[:i]) for i in range(sum_parts)]
    tall = chunk_of(hidden)
    bits = chips.bit_length() - 1

    def mirror(i):
        return sum((i // 2**p) % 2 * 2 ** (bits - 1 - p) for p in range(bits))

    spots = (chip, mirror(chip))
    halves = [chips >> (s + 1) for s in range(bits)]
    starts = [sum(halves[:s]) for s in range(bits)]

    def span(d, s, other):
        h = halves[s]
        side = lax.rem(spots[d] // h, 2)
        low = spots[d] // h * h
        return low + (h - 2 * h * side if other else 0)

    def peer(d, s):
        h = halves[s]
        spot = spots[d] + h - 2 * h * lax.rem(spots[d] // h, 2)
        return (mirror(spot) if d else spot) * 2 + core

    partner = dp + 1 - 2 * core

    barrier = pltpu.get_barrier_semaphore()
    for j in range(1, n):
        pl.semaphore_signal(
            barrier, inc=1, device_id=(dp, lax.rem(me + j, n)), device_id_type=MESH
        )
    for j in range(1, dp_size):
        pl.semaphore_signal(
            barrier, inc=1, device_id=(lax.rem(dp + j, dp_size), me), device_id_type=MESH
        )
    pl.semaphore_wait(barrier, n - 1 + dp_size - 1)

    def send(src, dst, s, r, to):
        return pltpu.make_async_remote_copy(
            src_ref=src, dst_ref=dst, send_sem=s, recv_sem=r, device_id=to, device_id_type=MESH
        )

    pending = []

    def start(cond, make, keep=True):
        if cond is None:
            make().start()
        else:

            @pl.when(cond)
            def _():
                make().start()

        if keep:
            pending.append((cond, make))

    def group(ref, s, r):
        return send(ref, ref, s, r, (partner, me))

    ways = (0, 1)
    step_of = (1, -1)
    room = (me, n - 1 - me)
    ahead = (n - 1 - me, me)

    def block_rows(b):
        return pl.ds(pl.multiple_of(b * tokens, tokens), tokens)

    loads = [
        pltpu.make_async_copy(x_hbm, xpad.at[pl.ds(EDGE, tokens)], ls.at[0]),
        pltpu.make_async_copy(wout_hbm, wout_ref, ls.at[1]),
        pltpu.make_async_copy(win_hbm, win_ref, ls.at[2]),
    ]

    def load_hidden(b):
        at = pl.ds(b * tokens, tokens)
        return pltpu.make_async_copy(h_hbm.at[at], h_ref.at[at], hl.at[b])

    def load_up(c):
        src = up_hbm.at[:, pl.ds(up_at[c], up_wide[c])]
        return pltpu.make_async_copy(src, gathers[c].at[block_rows(me)], ul.at[c])

    def place(k, b):
        return gathers[k].at[block_rows(b)]

    def source(k, b, own):
        if own and k < up_parts:
            return up_hbm.at[:, pl.ds(up_at[k], up_wide[k])]
        return place(k, b)

    def chain(k, d, back):
        b = jnp.clip(me - step_of[d] * back, 0, n - 1)
        to = (dp, jnp.clip(me + step_of[d], 0, n - 1))
        return send(source(k, b, back == 0), place(k, b), us.at[k, d], ur.at[k, b], to)

    def far(k, d):
        to = (dp, jnp.clip(me + 2 * step_of[d], 0, n - 1))
        return send(source(k, me, True), place(k, me), us.at[k, d], ur.at[k, me], to)

    def far_used(k):
        return k < FAR

    def own_send(k, d, cond):
        start(cond & (ahead[d] > 0), functools.partial(chain, k, d, 0), False)
        if far_used(k):
            start(cond & (room[d] == 0) & (ahead[d] > 1), functools.partial(far, k, d), False)

    def free(k):
        return 1 if far_used(k) else 0

    def later(k):
        if k == up_parts - 1:
            return range(up_parts, min(up_parts + LOOK, parts))
        if k + LOOK < up_parts or up_parts <= k < parts - LOOK:
            return [k + LOOK]
        return []

    def sent_of(m, k, d):
        front, behind = (n - 1 - m, m) if d == 0 else (m, n - 1 - m)
        if front == 0:
            return 0
        count = 1 + (far_used(k) and behind == 0 and front > 1)
        return count + sum(
            behind >= back and not (far_used(k) and back == 1 and behind == 1)
            for back in range(1, n - 1)
        )

    def x_edge(d):
        to = (dp, jnp.clip(me + step_of[d], 0, n - 1))
        src = x_hbm.at[pl.ds(tokens - EDGE if d == 0 else 0, EDGE)]
        dst = xpad.at[pl.ds(0 if d == 0 else EDGE + tokens, EDGE)]
        return send(src, dst, hs.at[d], hr.at[d], to)

    for d in ways:
        start(ahead[d] > 0, functools.partial(x_edge, d))
    for k in range(LOOK):
        for d in ways:
            own_send(k, d, me >= 0)
    for k in range(LOOK, up_parts):
        for d in ways:
            own_send(k, d, room[d] <= free(k))
    load_hidden(0).start()
    loads[0].start()
    for j in range(1, n):
        load_hidden(j).start()
    for c in range(up_parts):
        load_up(c).start()
    for load in loads[1:]:
        load.start()

    if act.shape[1] > hidden:
        act[:, pl.ds(hidden, act.shape[1] - hidden)] = jnp.zeros(
            (total_rows, act.shape[1] - hidden), BF16
        )
    bias[...] = jnp.zeros_like(bias)

    @pl.when(me == 0)
    def _():
        xpad[pl.ds(0, EDGE), :] = jnp.zeros((EDGE, width), BF16)
        gpad[pl.ds(0, EDGE), :] = jnp.zeros((EDGE, width), BF16)

    @pl.when(me == n - 1)
    def _():
        xpad[pl.ds(EDGE + tokens, EDGE), :] = jnp.zeros((EDGE, width), BF16)
        gpad[pl.ds(EDGE + tokens, EDGE), :] = jnp.zeros((EDGE, width), BF16)

    @scoped
    def gelu(b):
        load_hidden(b).wait()

        def gelu_step(i, _):
            at = pl.ds(pl.multiple_of(b * tokens + i * 32, 32), 32)
            v = h_ref[at, :].astype(F32)
            cdf = 0.5 + 0.5 * lax.erf(v * 0.7071067811865476)
            act[at, pl.ds(0, hidden)] = (v * cdf).astype(BF16)
            gh[at, :] = (cdf + v * (0.3989422804014327 * jnp.exp(-0.5 * v * v))).astype(BF16)
            return 0

        lax.fori_loop(0, tokens // 32, gelu_step, 0)

    @scoped
    def mix():
        for c in range(mix_parts):

            def mix_step(i, _, c=c):
                lane = pl.ds(pl.multiple_of(i * 128, 128), 128)
                at = pl.ds(pl.multiple_of(mix_at[c] + i * 128, 128), 128)
                x = xpad[:, at].astype(F32)
                taps = k_ref[:, at]
                total = x[EDGE : EDGE + tokens]
                for tap in range(KW):
                    low = EDGE - 3 + tap
                    total = total + taps[tap : tap + 1] * x[low : low + tokens]
                gathers[up_parts + c][block_rows(me), lane] = total.astype(BF16)
                return 0

            lax.fori_loop(0, mix_wide[c] // 128, mix_step, 0)

    @scoped
    def grad_dot(w):
        if w < up_parts:
            left, right = act, gathers[w]
        else:
            left, right = gathers[w], gh
        high = 2 * chips * rows_of[w]
        for half in (1 - core, core):
            lane = pl.ds(pl.multiple_of(half * high, 128), high)
            value = dot(left[:, lane], right[...], ((0,), (0,)))
            if half is core:
                accs[w][...] = value
            else:
                psends[w][...] = value.astype(BF16)
                start(None, functools.partial(pair_copy, w))

    batch = tokens * max(g for g in range(1, n + 1) if n % g == 0 and tokens * g <= ROWS)

    @scoped
    def back_dot():
        def back_step(i, _):
            at = pl.ds(pl.multiple_of(i * tall, tall), tall) if tall < hidden else pl.ds(0, hidden)

            def group_step(g, _):
                row = pl.ds(pl.multiple_of(g * batch, batch), batch)
                back = None
                for c in range(up_parts):
                    term = dot(
                        gathers[c][row, :], wout_ref[at, pl.ds(up_at[c], up_wide[c])], ((1,), (1,))
                    )
                    back = term if back is None else back + term
                grad = (gh[row, at].astype(F32) * back).astype(BF16)
                gh[row, at] = grad
                bias[:, at] += jnp.sum(grad.astype(F32), axis=0, keepdims=True)
                return 0

            if batch == total_rows:
                group_step(0, 0)
            else:
                lax.fori_loop(0, total_rows // batch, group_step, 0)
            return 0

        lax.fori_loop(0, hidden // tall, back_step, 0)

    @scoped
    def part_dot(r, count):
        at = pl.ds(sum_at[r], sum(sum_wide[r : r + count]))

        def group_step(g, _):
            row = pl.ds(pl.multiple_of(g * batch, batch), batch)
            value = dot(gh[row, :], win_ref[at, :], ((1,), (1,))).astype(BF16)
            for j in range(r, r + count):
                low = sum_at[j] - sum_at[r]
                sums[j][row, :] = value[:, low : low + sum_wide[j]]
            return 0

        if batch == total_rows:
            group_step(0, 0)
        else:
            lax.fori_loop(0, total_rows // batch, group_step, 0)

    def rows_at(w, d, block):
        return pl.ds(pl.multiple_of((d * chips + block) * rows_of[w], 8), rows_of[w])

    def pair_copy(w):
        return send(psends[w], precvs[w], ps.at[w], pr.at[w], (partner, me))

    def own(w, d, block):
        at = rows_at(w, d, block)
        return accs[w][at, :] + precvs[w][at, :].astype(F32)

    def ring_reduce(w, d, s):
        at = pl.ds(starts[s], halves[s])
        return send(
            rsends[w].at[d, at], rrecvs[w].at[d, at], rs.at[w], rr.at[w, s],
            (peer(d, s), me),
        )

    def ring_gather(w, d, s, other):
        ref = finals[w].at[core, d, pl.ds(span(d, s, other), halves[s])]
        at = 2 * bits - 1 - s
        return send(ref, ref, rs.at[w], rr.at[w, at], (peer(d, s), me))

    def across(w, d, s, half):
        if s == bits:
            ref = finals[w].at[half, d, pl.ds(spots[d], 1)]
        else:
            ref = finals[w].at[half, d, pl.ds(span(d, s, True), halves[s])]
        return send(ref, ref, ds.at[w], dr.at[w], (partner, me))

    last = 2 * bits

    @scoped
    def ring_step(w, s):
        acc, rsend, rrecv, final = accs[w], rsends[w], rrecvs[w], finals[w]
        if s == 0:
            pair_copy(w).wait_recv()
        else:
            j = s - 1 if s <= bits else 2 * bits - s
            both = rrecv.at[:, pl.ds(starts[j], halves[j])]
            group(both, rs.at[w], rr.at[w, s - 1]).wait_recv()
        for d in ways:
            if s <= bits:

                def value(block, s=s, d=d):
                    if s == 0:
                        return own(w, d, block)
                    got = rrecv[d, starts[s - 1] + block - span(d, s - 1, False)].astype(F32)
                    if s == 1:
                        return own(w, d, block) + got
                    return acc[rows_at(w, d, block), :] + got

                if s == bits:
                    final[core, d, spots[d]] = value(spots[d]).astype(BF16)
                    start(None, functools.partial(ring_gather, w, d, s - 1, False), False)
                    start(None, functools.partial(across, w, d, bits, core), False)
                    continue
                for j in range(halves[s]):
                    rsend[d, starts[s] + j] = value(span(d, s, True) + j).astype(BF16)
                start(None, functools.partial(ring_reduce, w, d, s), False)
                if s > 0:
                    for j in range(halves[s]):
                        block = span(d, s, False) + j
                        acc[rows_at(w, d, block), :] = value(block)
            else:
                step = 2 * bits - s
                if step > 0:
                    start(None, functools.partial(ring_gather, w, d, step - 1, False), False)
                start(None, functools.partial(across, w, d, step, core), False)

    @scoped
    def ring_end(w):
        group(finals[w].at[1 - core], ds.at[w], dr.at[w]).wait_recv()

    def target(d, t, behind):
        place = room[d] - behind
        block = n - 1 - t + place
        return block if d == 0 else n - 1 - block

    def z_slot(d, block, owner):
        return jnp.where((block == owner) & (d == 1), n, block)

    def z_send(r, d, t):
        block = jnp.clip(target(d, t, 0), 0, n - 1)
        to = jnp.clip(me + step_of[d], 0, n - 1)
        return send(
            sums[r].at[block_rows(block)], zrecvs[r].at[z_slot(d, block, to)],
            zs.at[r], zr.at[r, z_slot(d, block, to)], (dp, to),
        )

    def z_arrive(r, d, t):
        block = jnp.clip(target(d, t, 1), 0, n - 1)
        slot = z_slot(d, block, me)
        return group(zrecvs[r].at[slot], zs.at[r], zr.at[r, slot])

    @scoped
    def z_step(r, t):
        for d in ways:
            if t > 0:

                @pl.when((room[d] >= 1) & (room[d] - 1 <= t - 1))
                def _(d=d):
                    z_arrive(r, d, t - 1).wait_recv()
                    if t < n - 1:
                        block = jnp.clip(target(d, t - 1, 1), 0, n - 1)
                        at = block_rows(block)
                        sums[r][at, :] = (
                            sums[r][at, :].astype(F32) + zrecvs[r][z_slot(d, block, me)].astype(F32)
                        ).astype(BF16)

            if t < n - 1:
                start(
                    (room[d] <= t) & (room[d] > 0) & (ahead[d] > 0),
                    functools.partial(z_send, r, d, t),
                    False,
                )

    def z_first(r, t):
        for d in ways:
            start((room[d] == 0) & (ahead[d] > 0), functools.partial(z_send, r, d, t), False)

    active = []

    def tick(count=1):
        for _ in range(count):
            for item in list(active):
                ring_step(item[0], item[1])
                item[1] += 1
                if item[1] > last:
                    active.remove(item)

    def relays(k, d, back):
        go = (room[d] >= back) & (ahead[d] > 0)
        return go & (room[d] > 1) if far_used(k) and back == 1 else go

    @scoped
    def forward(k):
        for back in range(1, n):
            for d in ways:
                if back < n - 1:

                    @pl.when(relays(k, d, back))
                    def _(d=d):
                        chain(k, d, back).wait_recv()

                    start(relays(k, d, back), functools.partial(chain, k, d, back), False)
                for j in later(k):
                    own_send(j, d, (room[d] == back) & (room[d] > free(j)))

    @scoped
    def arrive(k):
        for back in range(1, n):
            for d in ways:

                @pl.when((room[d] >= back) & jnp.logical_not(relays(k, d, back)))
                def _(d=d):
                    chain(k, d, back).wait_recv()

    gelu(0)
    loads[0].wait()
    for d in ways:

        @pl.when(room[d] > 0)
        def _(d=d):
            x_edge(d).wait_recv()

    mix()
    for k in range(up_parts, parts):
        for d in ways:
            own_send(k, d, room[d] <= free(k))
    for b in range(1, n):
        gelu(b)
    for c in range(up_parts):
        load_up(c).wait()

    def bias_send(j):
        to = lax.rem(dp + j, dp_size)
        return send(kb.at[dp], kb.at[dp], kbs.at[0], kbr.at[0], (to, me))

    def bias_group():
        return group(kb.at[pl.ds(0, dp_size - 1)], kbs.at[0], kbr.at[0])

    sent = 0

    def relay_to(k):
        nonlocal sent
        while sent < min(k, parts):
            forward(sent)
            sent += 1

    def grad(k):
        arrive(k)
        grad_dot(k)
        tick()
        active.append([k, 1])
        ring_step(k, 0)

    for k in range(up_parts):
        relay_to(k + 1)
        if k == up_parts - 1:
            loads[1].wait()
            loads[2].wait()
        grad(k)
    relay_to(up_parts + 2)
    back_dot()
    kb[dp] = bias[...]
    for j in range(1, dp_size):
        start(None, functools.partial(bias_send, j), False)
    for r in range(0, sum_parts, 2):
        count = min(2, sum_parts - r)
        if r + 2 >= sum_parts:
            grad(up_parts)
        part_dot(r, count)
        for j in range(r, r + count):
            z_first(j, 0)
    for t in range(1, n - 1):
        for r in range(sum_parts):
            z_first(r, t)
    relay_to(parts)
    items = [(r, t) for t in range(1, n - 1) for r in range(sum_parts)]
    done = 0
    for k in range(up_parts, parts):
        if k > up_parts or sum_parts < 3:
            grad(k)
        goal = len(items) * (k - up_parts + 1) // max(1, mix_parts - 1)
        for item in items[done:goal]:
            z_step(*item)
        done = max(done, min(goal, len(items)))

    def g_edge(r, d):
        to = (dp, jnp.clip(me + step_of[d], 0, n - 1))
        lane = pl.ds(sum_at[r], sum_wide[r])
        src = gpad.at[pl.ds(tokens if d == 0 else EDGE, EDGE), lane]
        dst = gpad.at[pl.ds(0 if d == 0 else EDGE + tokens, EDGE), lane]
        return send(src, dst, gs.at[r, d], gr.at[r, d], to)

    @scoped
    def total_grad(r):
        edges = sorted({e for e in up_at + [width] if sum_at[r] < e < sum_at[r] + sum_wide[r]})
        edges = [sum_at[r]] + edges + [sum_at[r] + sum_wide[r]]
        for low, top in zip(edges, edges[1:]):
            c = max(i for i in range(up_parts) if up_at[i] <= low)

            def sum_step(i, _, low=low, c=c):
                at = pl.ds(pl.multiple_of(low + i * 128, 128), 128)
                lane = pl.ds(pl.multiple_of(low - sum_at[r] + i * 128, 128), 128)
                up_lane = pl.ds(pl.multiple_of(low - up_at[c] + i * 128, 128), 128)
                up = gathers[c][block_rows(me), up_lane].astype(F32)
                mine = sums[r][block_rows(me), lane].astype(F32)
                left = jnp.where(me > 0, zrecvs[r][me, :, lane].astype(F32), 0.0)
                right = jnp.where(me < n - 1, zrecvs[r][n, :, lane].astype(F32), 0.0)
                g = (up + (mine + left + right)).astype(BF16)
                gpad[pl.ds(EDGE, tokens), at] = g
                return 0

            lax.fori_loop(0, (top - low) // 128, sum_step, 0)
        for d in ways:
            start(ahead[d] > 0, functools.partial(g_edge, r, d))

    @scoped
    def taps(r):
        def taps_step(i, _):
            at = pl.ds(pl.multiple_of(sum_at[r] + i * 128, 128), 128)
            g = gpad[pl.ds(EDGE, tokens), at].astype(F32)
            x = xpad[:, at].astype(F32)
            totals = [
                jnp.sum(g * x[EDGE - 3 + tap : EDGE - 3 + tap + tokens], axis=0, keepdims=True)
                for tap in range(KW)
            ]
            totals.append(jnp.zeros_like(totals[0]))
            j = i + sum_at[r] // 128
            lane = pl.ds(pl.multiple_of(lax.rem(j, width // 256) * 128, 128), 128)
            kp[j // (width // 256), :, lane] = jnp.concatenate(totals, axis=0)
            return 0

        lax.fori_loop(0, sum_wide[r] // 128, taps_step, 0)

    @scoped
    def gin(r):
        for d in ways:

            @pl.when(room[d] > 0)
            def _(d=d):
                g_edge(r, d).wait_recv()

        def gin_step(i, _):
            at = pl.ds(pl.multiple_of(sum_at[r] + i * 128, 128), 128)
            g = gpad[:, at].astype(F32)
            taps = k_ref[:, at]
            total = g[EDGE : EDGE + tokens]
            for tap in range(KW):
                low = EDGE + 3 - tap
                total = total + taps[tap : tap + 1] * g[low : low + tokens]
            gin_ref[:, at] = total.astype(BF16)
            return 0

        lax.fori_loop(0, sum_wide[r] // 128, gin_step, 0)

    for r in range(sum_parts):
        z_step(r, n - 1)
        total_grad(r)
        taps(r)
        if r == 1:
            tick()

    def pair_taps():
        return send(kp.at[1 - core], kp.at[2], kps.at[0], kpr.at[0], (partner, me))

    start(None, pair_taps)
    tick()
    for r in range(sum_parts - 1):
        gin(r)

    def k1_send(j):
        to = lax.rem(me + j, n)
        return send(k1.at[me], k1.at[me], k1s.at[0], k1r.at[0], (dp, to))

    def k1_group():
        return group(k1.at[pl.ds(0, n - 1)], k1s.at[0], k1r.at[0])

    pair_taps().wait_recv()
    k1[me] = kp[core] + kp[2]
    for j in range(1, n):
        start(None, functools.partial(k1_send, j), False)
    tick()
    gin(sum_parts - 1)

    @scoped
    def k1_wait():
        k1_group().wait_recv()

    k1_wait()
    taps_sum = k1[0]
    for j in range(1, n):
        taps_sum = taps_sum + k1[j]
    k2[chip] = taps_sum

    def k2_send(j):
        to = lax.rem(chip + j, chips) * 2 + core
        return send(k2.at[chip], k2.at[chip], k2s.at[0], k2r.at[0], (to, me))

    def k2_group():
        return group(k2.at[pl.ds(0, chips - 1)], k2s.at[0], k2r.at[0])

    for j in range(1, chips):
        start(None, functools.partial(k2_send, j), False)
    tick()

    @scoped
    def k2_wait():
        k2_group().wait_recv()

    k2_wait()
    total = k2[0]
    for j in range(1, chips):
        total = total + k2[j]
    k3[core] = total

    def k3_copy(half):
        return send(k3.at[half], k3.at[half], k3s.at[0], k3r.at[0], (partner, me))

    start(None, functools.partial(k3_copy, core))
    while active:
        tick()
    bias_group().wait_recv()
    total = kb[0]
    for j in range(1, dp_size):
        total = total + kb[j]
    gb_ref[...] = total
    k3_copy(1 - core).wait_recv()
    for half in range(2):
        gk_ref[:, pl.ds(half * (width // 2), width // 2)] = k3[half, :KW]
    for w in range(parts):
        ring_end(w)

    @scoped
    def drain():
        for m in range(n):

            @pl.when(me == m)
            def _(m=m):
                for k in range(parts):
                    for d in ways:
                        count = sent_of(m, k, d)
                        if count:
                            ref = gathers[k].at[pl.ds(0, count * tokens)]
                            group(ref, us.at[k, d], ur.at[k, 0]).wait_send()

        for w in range(parts):
            group(finals[w].at[:, :, pl.ds(0, chips - 1)], rs.at[w], rr.at[w, 0]).wait_send()
            group(finals[w].at[1 - core], ds.at[w], dr.at[w]).wait_send()
        for r in range(sum_parts):
            ref = sums[r].at[pl.ds(0, (n - 1) * tokens)]
            group(ref, zs.at[r], zr.at[r, 0]).wait_send()
        bias_group().wait_send()
        k1_group().wait_send()
        k2_group().wait_send()
        for cond, make in pending:
            if cond is None:
                make().wait_send()
            else:

                @pl.when(cond)
                def _(make=make):
                    make().wait_send()

    drain()


def shards(n, dp_size, inputs, saved_hidden, upstream, w_in, w_out, kernel):
    chips = dp_size // 2
    tokens, width = inputs.shape[1:]
    hidden = w_in.shape[1]
    total_rows = n * tokens
    up_wide = cuts(width, 256, UP_SHARES)
    mix_wide = cuts(width, 64 * chips, MIX_SHARES)
    sum_wide = cuts(width, 256, SUM_SHARES)
    up_parts, mix_parts, sum_parts = len(up_wide), len(mix_wide), len(sum_wide)
    parts = up_parts + mix_parts
    rows_out = -(-hidden // (4 * chips * 8)) * 8
    high = rows_out * 4 * chips
    rows_of = [rows_out] * up_parts + [wide // (4 * chips) for wide in mix_wide]
    sizes = [(rows_out, wide) for wide in up_wide] + [
        (rows, hidden) for rows in rows_of[up_parts:]
    ]
    dma = pltpu.SemaphoreType.DMA
    bits = chips.bit_length() - 1
    vmem = pl.BlockSpec(memory_space=pltpu.VMEM)
    hbm = pl.BlockSpec(memory_space=pltpu.HBM)
    shape = jax.ShapeDtypeStruct
    grad_inputs, grad_kernel, grad_bias, *finals = pl.pallas_call(
        functools.partial(body, n, dp_size, up_wide, mix_wide, sum_wide, rows_of),
        out_shape=[shape((tokens, width), BF16), shape((KW, width), F32), shape((1, hidden), F32)]
        + [shape((2, 2, chips) + size, BF16) for size in sizes],
        in_specs=[hbm] * 5 + [vmem],
        out_specs=[vmem] * (3 + parts),
        scratch_shapes=[pltpu.VMEM((2 * chips * r, c), F32) for r, c in sizes]
        + [pltpu.VMEM((2 * chips * r, c), BF16) for r, c in sizes] * 2
        + [pltpu.VMEM((2, chips - 1) + size, BF16) for size in sizes] * 2
        + [pltpu.VMEM((total_rows, wide), BF16) for wide in up_wide + mix_wide]
        + [pltpu.VMEM((total_rows, wide), BF16) for wide in sum_wide]
        + [pltpu.VMEM((n + 1, tokens, wide), BF16) for wide in sum_wide]
        + [
            pltpu.VMEM((total_rows, hidden), BF16),
            pltpu.VMEM((width, hidden), BF16),
            pltpu.VMEM((hidden, width), BF16),
            pltpu.VMEM((total_rows, high), BF16),
            pltpu.VMEM((total_rows, hidden), BF16),
            pltpu.VMEM((tokens + 2 * EDGE, width), BF16),
            pltpu.VMEM((tokens + 2 * EDGE, width), BF16),
            pltpu.VMEM((1, hidden), F32),
            pltpu.VMEM((dp_size, 1, hidden), F32),
            pltpu.VMEM((3, 8, width // 2), F32),
            pltpu.VMEM((n, 8, width // 2), F32),
            pltpu.VMEM((chips, 8, width // 2), F32),
            pltpu.VMEM((2, 8, width // 2), F32),
            dma((3,)), dma((n,)), dma((up_parts,)),
            dma((2,)), dma((2,)),
            dma((parts, 2)), dma((parts, n)),
            dma((sum_parts,)), dma((sum_parts, n + 1)),
            dma((parts,)), dma((parts,)),
            dma((parts,)), dma((parts, 2 * bits)),
            dma((parts,)), dma((parts,)),
            dma((sum_parts, 2)), dma((sum_parts, 2)),
            dma((1,)), dma((1,)),
            dma((1,)), dma((1,)),
            dma((1,)), dma((1,)),
            dma((1,)), dma((1,)),
            dma((1,)), dma((1,)),
        ],
        compiler_params=pltpu.CompilerParams(
            collective_id=0, has_side_effects=True, vmem_limit_bytes=VMEM if total_rows <= ROWS else 67043328
        ),
    )(
        inputs[0],
        saved_hidden[0],
        upstream[0],
        w_in,
        w_out,
        kernel,
    )
    outs = [f.reshape(high, wide) for f, wide in zip(finals, up_wide)]
    outs += [f.reshape(wide, hidden) for f, wide in zip(finals[up_parts:], mix_wide)]
    return tuple(
        pl.pallas_call(
            functools.partial(widen, up_wide, mix_wide),
            out_shape=[
                shape((1, tokens, width), BF16),
                shape((width, hidden), F32),
                shape((hidden, width), F32),
                shape((hidden,), F32),
                shape((KW, width), F32),
            ],
            in_specs=[vmem] * (parts + 3),
            out_specs=[hbm] * 3 + [vmem] + [hbm],
            scratch_shapes=[pltpu.VMEM((wide, hidden), F32) for wide in mix_wide]
            + [pltpu.VMEM((hidden, wide), F32) for wide in up_wide]
            + [dma((parts + 2,))],
            compiler_params=pltpu.CompilerParams(vmem_limit_bytes=24 * 2**20),
        )(*outs, grad_inputs, grad_kernel, grad_bias)
    )


def widen(up_wide, mix_wide, *refs):
    up_parts, mix_parts = len(up_wide), len(mix_wide)
    parts = up_parts + mix_parts
    finals, (gin, gk, gb), refs = refs[:parts], refs[parts : parts + 3], refs[parts + 3 :]
    gin_out, rows_out, cols_out, gb_out, gk_out, *refs = refs
    rows, cols, sem = refs[:mix_parts], refs[mix_parts:-1], refs[-1]
    copies = [
        pltpu.make_async_copy(gin, gin_out.at[0], sem.at[parts]),
        pltpu.make_async_copy(gk, gk_out, sem.at[parts + 1]),
    ]
    for copy in copies:
        copy.start()
    gb_out[...] = gb[0]

    def widen_one(source, target):
        high = target.shape[0]
        step = 128

        def widen_step(i, _):
            at = pl.ds(pl.multiple_of(i * step, step), step)
            target[at, :] = source[at, :].astype(F32)
            return 0

        lax.fori_loop(0, high // step, widen_step, 0)

    for c in range(mix_parts):
        widen_one(finals[up_parts + c], rows[c])
        at = pl.ds(sum(mix_wide[:c]), mix_wide[c])
        copies.append(pltpu.make_async_copy(rows[c], rows_out.at[at], sem.at[c]))
        copies[-1].start()
    for c in range(up_parts):
        widen_one(finals[c], cols[c])
        at = pl.ds(sum(up_wide[:c]), up_wide[c])
        copies.append(pltpu.make_async_copy(cols[c], cols_out.at[:, at], sem.at[mix_parts + c]))
        copies[-1].start()
    for copy in copies:
        copy.wait()


def solution(mesh):
    in_specs = (
        P("dp", "tp", None),
        P("dp", None, "tp"),
        P("dp", "tp", None),
        P(None, "tp"),
        P("tp", None),
        P(),
    )
    out_specs = (P("dp", "tp", None), P(None, "tp"), P("tp", None), P("tp"), P())
    return jax.shard_map(
        functools.partial(shards, mesh.shape["tp"], mesh.shape["dp"]),
        mesh=mesh,
        in_specs=in_specs,
        out_specs=out_specs,
        check_vma=False,
    )
```

```python
import functools

import jax
import jax.numpy as jnp
from jax import lax
from jax.experimental import pallas as pl
from jax.experimental.pallas import tpu as pltpu
from jax.sharding import PartitionSpec as P

KW = 7
EDGE = 16
ROWS = 768
FAR = 10
LOOK = 2
VMEM = 45 * 2**20
UP_SHARES = (1,) * 5
MIX_SHARES = (1,) * 5
SUM_SHARES = (1,) * 5
F32 = jnp.float32
BF16 = jnp.bfloat16
MESH = pl.DeviceIdType.MESH


def dot(a, b, dims):
    return lax.dot_general(a, b, (dims, ((), ())), preferred_element_type=F32)


def chunk_of(size):
    return 256 if size % 256 == 0 else size


def scoped(function):
    def wrapped(*args):
        with jax.named_scope(function.__name__ + "".join(f"_{a}" for a in args if isinstance(a, int))):
            return function(*args)

    return wrapped


def cuts(width, unit, shares):
    if width % unit or width // unit < len(shares):
        return [width]
    units = width // unit
    total = sum(shares)
    edges = [units * sum(shares[:i]) // total for i in range(len(shares) + 1)]
    return [(b - a) * unit for a, b in zip(edges, edges[1:])]


def body(
    n, dp_size, up_wide, mix_wide, sum_wide, rows_of,
    x_hbm, h_hbm, up_hbm, win_hbm, wout_hbm, k_ref, gin_ref, gk_ref, gb_ref, *refs,
):
    def take(count):
        nonlocal refs
        got, refs = refs[:count], refs[count:]
        return got

    up_parts, mix_parts, sum_parts = len(up_wide), len(mix_wide), len(sum_wide)
    parts = up_parts + mix_parts
    finals = take(parts)
    accs = take(parts)
    psends = take(parts)
    precvs = take(parts)
    rsends = take(parts)
    rrecvs = take(parts)
    gathers = take(parts)
    sums = take(sum_parts)
    zrecvs = take(sum_parts)
    (
        h_ref, win_ref, wout_ref, act, gh, xpad, gpad, bias, kb, kp, k1, k2, k3,
        ls, hl, ul, hs, hr, us, ur, zs, zr, ps, pr, rs, rr, ds, dr, gs, gr,
        kbs, kbr, kps, kpr, k1s, k1r, k2s, k2r, k3s, k3r,
    ) = refs
    chips = dp_size // 2
    me = lax.axis_index("tp")
    dp = lax.axis_index("dp")
    core = lax.rem(dp, 2)
    chip = dp // 2
    tokens, width = x_hbm.shape
    total_rows, hidden = h_ref.shape
    up_at = [sum(up_wide[:i]) for i in range(up_parts)]
    mix_at = [sum(mix_wide[:i]) for i in range(mix_parts)]
    sum_at = [sum(sum_wide[:i]) for i in range(sum_parts)]
    tall = chunk_of(hidden)
    bits = chips.bit_length() - 1

    def mirror(i):
        return sum((i // 2**p) % 2 * 2 ** (bits - 1 - p) for p in range(bits))

    spots = (chip, mirror(chip))
    halves = [chips >> (s + 1) for s in range(bits)]
    starts = [sum(halves[:s]) for s in range(bits)]

    def span(d, s, other):
        h = halves[s]
        side = lax.rem(spots[d] // h, 2)
        low = spots[d] // h * h
        return low + (h - 2 * h * side if other else 0)

    def peer(d, s):
        h = halves[s]
        spot = spots[d] + h - 2 * h * lax.rem(spots[d] // h, 2)
        return (mirror(spot) if d else spot) * 2 + core

    partner = dp + 1 - 2 * core

    barrier = pltpu.get_barrier_semaphore()
    for j in range(1, n):
        pl.semaphore_signal(
            barrier, inc=1, device_id=(dp, lax.rem(me + j, n)), device_id_type=MESH
        )
    for j in range(1, dp_size):
        pl.semaphore_signal(
            barrier, inc=1, device_id=(lax.rem(dp + j, dp_size), me), device_id_type=MESH
        )
    pl.semaphore_wait(barrier, n - 1 + dp_size - 1)

    def send(src, dst, s, r, to):
        return pltpu.make_async_remote_copy(
            src_ref=src, dst_ref=dst, send_sem=s, recv_sem=r, device_id=to, device_id_type=MESH
        )

    pending = []

    def start(cond, make, keep=True):
        if cond is None:
            make().start()
        else:

            @pl.when(cond)
            def _():
                make().start()

        if keep:
            pending.append((cond, make))

    def group(ref, s, r):
        return send(ref, ref, s, r, (partner, me))

    ways = (0, 1)
    step_of = (1, -1)
    room = (me, n - 1 - me)
    ahead = (n - 1 - me, me)

    def block_rows(b):
        return pl.ds(pl.multiple_of(b * tokens, tokens), tokens)

    loads = [
        pltpu.make_async_copy(x_hbm, xpad.at[pl.ds(EDGE, tokens)], ls.at[0]),
        pltpu.make_async_copy(wout_hbm, wout_ref, ls.at[1]),
        pltpu.make_async_copy(win_hbm, win_ref, ls.at[2]),
    ]

    def load_hidden(b):
        at = pl.ds(b * tokens, tokens)
        return pltpu.make_async_copy(h_hbm.at[at], h_ref.at[at], hl.at[b])

    def load_up(c):
        src = up_hbm.at[:, pl.ds(up_at[c], up_wide[c])]
        return pltpu.make_async_copy(src, gathers[c].at[block_rows(me)], ul.at[c])

    def place(k, b):
        return gathers[k].at[block_rows(b)]

    def source(k, b, own):
        if own and k < up_parts:
            return up_hbm.at[:, pl.ds(up_at[k], up_wide[k])]
        return place(k, b)

    def chain(k, d, back):
        b = jnp.clip(me - step_of[d] * back, 0, n - 1)
        to = (dp, jnp.clip(me + step_of[d], 0, n - 1))
        return send(source(k, b, back == 0), place(k, b), us.at[k, d], ur.at[k, b], to)

    def far(k, d):
        to = (dp, jnp.clip(me + 2 * step_of[d], 0, n - 1))
        return send(source(k, me, True), place(k, me), us.at[k, d], ur.at[k, me], to)

    def far_used(k):
        return k < FAR

    def own_send(k, d, cond):
        start(cond & (ahead[d] > 0), functools.partial(chain, k, d, 0), False)
        if far_used(k):
            start(cond & (room[d] == 0) & (ahead[d] > 1), functools.partial(far, k, d), False)

    def free(k):
        return 1 if far_used(k) else 0

    def later(k):
        if k == up_parts - 1:
            return range(up_parts, min(up_parts + LOOK, parts))
        if k + LOOK < up_parts or up_parts <= k < parts - LOOK:
            return [k + LOOK]
        return []

    def sent_of(m, k, d):
        front, behind = (n - 1 - m, m) if d == 0 else (m, n - 1 - m)
        if front == 0:
            return 0
        count = 1 + (far_used(k) and behind == 0 and front > 1)
        return count + sum(
            behind >= back and not (far_used(k) and back == 1 and behind == 1)
            for back in range(1, n - 1)
        )

    def x_edge(d):
        to = (dp, jnp.clip(me + step_of[d], 0, n - 1))
        src = x_hbm.at[pl.ds(tokens - EDGE if d == 0 else 0, EDGE)]
        dst = xpad.at[pl.ds(0 if d == 0 else EDGE + tokens, EDGE)]
        return send(src, dst, hs.at[d], hr.at[d], to)

    for d in ways:
        start(ahead[d] > 0, functools.partial(x_edge, d))
    for k in range(LOOK):
        for d in ways:
            own_send(k, d, me >= 0)
    for k in range(LOOK, up_parts):
        for d in ways:
            own_send(k, d, room[d] <= free(k))
    load_hidden(0).start()
    loads[0].start()
    for j in range(1, n):
        load_hidden(j).start()
    for c in range(up_parts):
        load_up(c).start()
    for load in loads[1:]:
        load.start()

    if act.shape[1] > hidden:
        act[:, pl.ds(hidden, act.shape[1] - hidden)] = jnp.zeros(
            (total_rows, act.shape[1] - hidden), BF16
        )
    bias[...] = jnp.zeros_like(bias)

    @pl.when(me == 0)
    def _():
        xpad[pl.ds(0, EDGE), :] = jnp.zeros((EDGE, width), BF16)
        gpad[pl.ds(0, EDGE), :] = jnp.zeros((EDGE, width), BF16)

    @pl.when(me == n - 1)
    def _():
        xpad[pl.ds(EDGE + tokens, EDGE), :] = jnp.zeros((EDGE, width), BF16)
        gpad[pl.ds(EDGE + tokens, EDGE), :] = jnp.zeros((EDGE, width), BF16)

    @scoped
    def gelu(b):
        load_hidden(b).wait()

        def gelu_step(i, _):
            at = pl.ds(pl.multiple_of(b * tokens + i * 32, 32), 32)
            v = h_ref[at, :].astype(F32)
            cdf = 0.5 + 0.5 * lax.erf(v * 0.7071067811865476)
            act[at, pl.ds(0, hidden)] = (v * cdf).astype(BF16)
            gh[at, :] = (cdf + v * (0.3989422804014327 * jnp.exp(-0.5 * v * v))).astype(BF16)
            return 0

        lax.fori_loop(0, tokens // 32, gelu_step, 0)

    @scoped
    def mix():
        for c in range(mix_parts):

            def mix_step(i, _, c=c):
                lane = pl.ds(pl.multiple_of(i * 128, 128), 128)
                at = pl.ds(pl.multiple_of(mix_at[c] + i * 128, 128), 128)
                x = xpad[:, at].astype(F32)
                taps = k_ref[:, at]
                total = x[EDGE : EDGE + tokens]
                for tap in range(KW):
                    low = EDGE - 3 + tap
                    total = total + taps[tap : tap + 1] * x[low : low + tokens]
                gathers[up_parts + c][block_rows(me), lane] = total.astype(BF16)
                return 0

            lax.fori_loop(0, mix_wide[c] // 128, mix_step, 0)

    @scoped
    def grad_dot(w):
        if w < up_parts:
            left, right = act, gathers[w]
        else:
            left, right = gathers[w], gh
        high = 2 * chips * rows_of[w]
        for half in (1 - core, core):
            lane = pl.ds(pl.multiple_of(half * high, 128), high)
            value = dot(left[:, lane], right[...], ((0,), (0,)))
            if half is core:
                accs[w][...] = value
            else:
                psends[w][...] = value.astype(BF16)
                start(None, functools.partial(pair_copy, w))

    batch = tokens * max(g for g in range(1, n + 1) if n % g == 0 and tokens * g <= ROWS)

    @scoped
    def back_dot():
        def back_step(i, _):
            at = pl.ds(pl.multiple_of(i * tall, tall), tall) if tall < hidden else pl.ds(0, hidden)

            def group_step(g, _):
                row = pl.ds(pl.multiple_of(g * batch, batch), batch)
                back = None
                for c in range(up_parts):
                    term = dot(
                        gathers[c][row, :], wout_ref[at, pl.ds(up_at[c], up_wide[c])], ((1,), (1,))
                    )
                    back = term if back is None else back + term
                grad = (gh[row, at].astype(F32) * back).astype(BF16)
                gh[row, at] = grad
                bias[:, at] += jnp.sum(grad.astype(F32), axis=0, keepdims=True)
                return 0

            if batch == total_rows:
                group_step(0, 0)
            else:
                lax.fori_loop(0, total_rows // batch, group_step, 0)
            return 0

        lax.fori_loop(0, hidden // tall, back_step, 0)

    @scoped
    def part_dot(r, count):
        at = pl.ds(sum_at[r], sum(sum_wide[r : r + count]))

        def group_step(g, _):
            row = pl.ds(pl.multiple_of(g * batch, batch), batch)
            value = dot(gh[row, :], win_ref[at, :], ((1,), (1,))).astype(BF16)
            for j in range(r, r + count):
                low = sum_at[j] - sum_at[r]
                sums[j][row, :] = value[:, low : low + sum_wide[j]]
            return 0

        if batch == total_rows:
            group_step(0, 0)
        else:
            lax.fori_loop(0, total_rows // batch, group_step, 0)

    def rows_at(w, d, block):
        return pl.ds(pl.multiple_of((d * chips + block) * rows_of[w], 8), rows_of[w])

    def pair_copy(w):
        return send(psends[w], precvs[w], ps.at[w], pr.at[w], (partner, me))

    def own(w, d, block):
        at = rows_at(w, d, block)
        return accs[w][at, :] + precvs[w][at, :].astype(F32)

    def ring_reduce(w, d, s):
        at = pl.ds(starts[s], halves[s])
        return send(
            rsends[w].at[d, at], rrecvs[w].at[d, at], rs.at[w], rr.at[w, s],
            (peer(d, s), me),
        )

    def ring_gather(w, d, s, other):
        ref = finals[w].at[core, d, pl.ds(span(d, s, other), halves[s])]
        at = 2 * bits - 1 - s
        return send(ref, ref, rs.at[w], rr.at[w, at], (peer(d, s), me))

    def across(w, d, s, half):
        if s == bits:
            ref = finals[w].at[half, d, pl.ds(spots[d], 1)]
        else:
            ref = finals[w].at[half, d, pl.ds(span(d, s, True), halves[s])]
        return send(ref, ref, ds.at[w], dr.at[w], (partner, me))

    last = 2 * bits

    @scoped
    def ring_step(w, s):
        acc, rsend, rrecv, final = accs[w], rsends[w], rrecvs[w], finals[w]
        if s == 0:
            pair_copy(w).wait_recv()
        else:
            j = s - 1 if s <= bits else 2 * bits - s
            both = rrecv.at[:, pl.ds(starts[j], halves[j])]
            group(both, rs.at[w], rr.at[w, s - 1]).wait_recv()
        for d in ways:
            if s <= bits:

                def value(block, s=s, d=d):
                    if s == 0:
                        return own(w, d, block)
                    got = rrecv[d, starts[s - 1] + block - span(d, s - 1, False)].astype(F32)
                    if s == 1:
                        return own(w, d, block) + got
                    return acc[rows_at(w, d, block), :] + got

                if s == bits:
                    final[core, d, spots[d]] = value(spots[d]).astype(BF16)
                    start(None, functools.partial(ring_gather, w, d, s - 1, False), False)
                    start(None, functools.partial(across, w, d, bits, core), False)
                    continue
                for j in range(halves[s]):
                    rsend[d, starts[s] + j] = value(span(d, s, True) + j).astype(BF16)
                start(None, functools.partial(ring_reduce, w, d, s), False)
                if s > 0:
                    for j in range(halves[s]):
                        block = span(d, s, False) + j
                        acc[rows_at(w, d, block), :] = value(block)
            else:
                step = 2 * bits - s
                if step > 0:
                    start(None, functools.partial(ring_gather, w, d, step - 1, False), False)
                start(None, functools.partial(across, w, d, step, core), False)

    @scoped
    def ring_end(w):
        group(finals[w].at[1 - core], ds.at[w], dr.at[w]).wait_recv()

    def target(d, t, behind):
        place = room[d] - behind
        block = n - 1 - t + place
        return block if d == 0 else n - 1 - block

    def z_slot(d, block, owner):
        return jnp.where((block == owner) & (d == 1), n, block)

    def z_send(r, d, t):
        block = jnp.clip(target(d, t, 0), 0, n - 1)
        to = jnp.clip(me + step_of[d], 0, n - 1)
        return send(
            sums[r].at[block_rows(block)], zrecvs[r].at[z_slot(d, block, to)],
            zs.at[r], zr.at[r, z_slot(d, block, to)], (dp, to),
        )

    def z_arrive(r, d, t):
        block = jnp.clip(target(d, t, 1), 0, n - 1)
        slot = z_slot(d, block, me)
        return group(zrecvs[r].at[slot], zs.at[r], zr.at[r, slot])

    @scoped
    def z_step(r, t):
        for d in ways:
            if t > 0:

                @pl.when((room[d] >= 1) & (room[d] - 1 <= t - 1))
                def _(d=d):
                    z_arrive(r, d, t - 1).wait_recv()
                    if t < n - 1:
                        block = jnp.clip(target(d, t - 1, 1), 0, n - 1)
                        at = block_rows(block)
                        sums[r][at, :] = (
                            sums[r][at, :].astype(F32) + zrecvs[r][z_slot(d, block, me)].astype(F32)
                        ).astype(BF16)

            if t < n - 1:
                start(
                    (room[d] <= t) & (room[d] > 0) & (ahead[d] > 0),
                    functools.partial(z_send, r, d, t),
                    False,
                )

    def z_first(r, t):
        for d in ways:
            start((room[d] == 0) & (ahead[d] > 0), functools.partial(z_send, r, d, t), False)

    active = []

    def tick(count=1):
        for _ in range(count):
            for item in list(active):
                ring_step(item[0], item[1])
                item[1] += 1
                if item[1] > last:
                    active.remove(item)

    def relays(k, d, back):
        go = (room[d] >= back) & (ahead[d] > 0)
        return go & (room[d] > 1) if far_used(k) and back == 1 else go

    @scoped
    def forward(k):
        for back in range(1, n):
            for d in ways:
                if back < n - 1:

                    @pl.when(relays(k, d, back))
                    def _(d=d):
                        chain(k, d, back).wait_recv()

                    start(relays(k, d, back), functools.partial(chain, k, d, back), False)
                for j in later(k):
                    own_send(j, d, (room[d] == back) & (room[d] > free(j)))

    @scoped
    def arrive(k):
        for back in range(1, n):
            for d in ways:

                @pl.when((room[d] >= back) & jnp.logical_not(relays(k, d, back)))
                def _(d=d):
                    chain(k, d, back).wait_recv()

    gelu(0)
    loads[0].wait()
    for d in ways:

        @pl.when(room[d] > 0)
        def _(d=d):
            x_edge(d).wait_recv()

    mix()
    for k in range(up_parts, parts):
        for d in ways:
            own_send(k, d, room[d] <= free(k))
    for b in range(1, n):
        gelu(b)
    for c in range(up_parts):
        load_up(c).wait()

    def bias_send(j):
        to = lax.rem(dp + j, dp_size)
        return send(kb.at[dp], kb.at[dp], kbs.at[0], kbr.at[0], (to, me))

    def bias_group():
        return group(kb.at[pl.ds(0, dp_size - 1)], kbs.at[0], kbr.at[0])

    sent = 0

    def relay_to(k):
        nonlocal sent
        while sent < min(k, parts):
            forward(sent)
            sent += 1

    def grad(k):
        arrive(k)
        grad_dot(k)
        tick()
        active.append([k, 1])
        ring_step(k, 0)

    for k in range(up_parts):
        relay_to(k + 1)
        if k == up_parts - 1:
            loads[1].wait()
            loads[2].wait()
        grad(k)
    relay_to(up_parts + 2)
    back_dot()
    kb[dp] = bias[...]
    for j in range(1, dp_size):
        start(None, functools.partial(bias_send, j), False)
    for r in range(0, sum_parts, 2):
        count = min(2, sum_parts - r)
        if r + 2 >= sum_parts:
            grad(up_parts)
        part_dot(r, count)
        for j in range(r, r + count):
            z_first(j, 0)
    for t in range(1, n - 1):
        for r in range(sum_parts):
            z_first(r, t)
    relay_to(parts)
    items = [(r, t) for t in range(1, n - 1) for r in range(sum_parts)]
    done = 0
    for k in range(up_parts, parts):
        if k > up_parts or sum_parts < 3:
            grad(k)
        goal = len(items) * (k - up_parts + 1) // max(1, mix_parts - 1)
        for item in items[done:goal]:
            z_step(*item)
        done = max(done, min(goal, len(items)))

    def g_edge(r, d):
        to = (dp, jnp.clip(me + step_of[d], 0, n - 1))
        lane = pl.ds(sum_at[r], sum_wide[r])
        src = gpad.at[pl.ds(tokens if d == 0 else EDGE, EDGE), lane]
        dst = gpad.at[pl.ds(0 if d == 0 else EDGE + tokens, EDGE), lane]
        return send(src, dst, gs.at[r, d], gr.at[r, d], to)

    @scoped
    def total_grad(r):
        edges = sorted({e for e in up_at + [width] if sum_at[r] < e < sum_at[r] + sum_wide[r]})
        edges = [sum_at[r]] + edges + [sum_at[r] + sum_wide[r]]
        for low, top in zip(edges, edges[1:]):
            c = max(i for i in range(up_parts) if up_at[i] <= low)

            def sum_step(i, _, low=low, c=c):
                at = pl.ds(pl.multiple_of(low + i * 128, 128), 128)
                lane = pl.ds(pl.multiple_of(low - sum_at[r] + i * 128, 128), 128)
                up_lane = pl.ds(pl.multiple_of(low - up_at[c] + i * 128, 128), 128)
                up = gathers[c][block_rows(me), up_lane].astype(F32)
                mine = sums[r][block_rows(me), lane].astype(F32)
                left = jnp.where(me > 0, zrecvs[r][me, :, lane].astype(F32), 0.0)
                right = jnp.where(me < n - 1, zrecvs[r][n, :, lane].astype(F32), 0.0)
                g = (up + (mine + left + right)).astype(BF16)
                gpad[pl.ds(EDGE, tokens), at] = g
                return 0

            lax.fori_loop(0, (top - low) // 128, sum_step, 0)
        for d in ways:
            start(ahead[d] > 0, functools.partial(g_edge, r, d))

    @scoped
    def taps(r):
        def taps_step(i, _):
            at = pl.ds(pl.multiple_of(sum_at[r] + i * 128, 128), 128)
            g = gpad[pl.ds(EDGE, tokens), at].astype(F32)
            x = xpad[:, at].astype(F32)
            totals = [
                jnp.sum(g * x[EDGE - 3 + tap : EDGE - 3 + tap + tokens], axis=0, keepdims=True)
                for tap in range(KW)
            ]
            totals.append(jnp.zeros_like(totals[0]))
            j = i + sum_at[r] // 128
            lane = pl.ds(pl.multiple_of(lax.rem(j, width // 256) * 128, 128), 128)
            kp[j // (width // 256), :, lane] = jnp.concatenate(totals, axis=0)
            return 0

        lax.fori_loop(0, sum_wide[r] // 128, taps_step, 0)

    @scoped
    def gin(r):
        for d in ways:

            @pl.when(room[d] > 0)
            def _(d=d):
                g_edge(r, d).wait_recv()

        def gin_step(i, _):
            at = pl.ds(pl.multiple_of(sum_at[r] + i * 128, 128), 128)
            g = gpad[:, at].astype(F32)
            taps = k_ref[:, at]
            total = g[EDGE : EDGE + tokens]
            for tap in range(KW):
                low = EDGE + 3 - tap
                total = total + taps[tap : tap + 1] * g[low : low + tokens]
            gin_ref[:, at] = total.astype(BF16)
            return 0

        lax.fori_loop(0, sum_wide[r] // 128, gin_step, 0)

    for r in range(sum_parts):
        z_step(r, n - 1)
        total_grad(r)
        taps(r)
        if r == 1:
            tick()

    def pair_taps():
        return send(kp.at[1 - core], kp.at[2], kps.at[0], kpr.at[0], (partner, me))

    start(None, pair_taps)
    for r in range(sum_parts - 1):
        gin(r)

    def k1_send(j):
        to = lax.rem(me + j, n)
        return send(k1.at[me], k1.at[me], k1s.at[0], k1r.at[0], (dp, to))

    def k1_group():
        return group(k1.at[pl.ds(0, n - 1)], k1s.at[0], k1r.at[0])

    pair_taps().wait_recv()
    k1[me] = kp[core] + kp[2]
    for j in range(1, n):
        start(None, functools.partial(k1_send, j), False)
    tick(2)
    gin(sum_parts - 1)

    @scoped
    def k1_wait():
        k1_group().wait_recv()

    k1_wait()
    taps_sum = k1[0]
    for j in range(1, n):
        taps_sum = taps_sum + k1[j]
    k2[chip] = taps_sum

    def k2_send(j):
        to = lax.rem(chip + j, chips) * 2 + core
        return send(k2.at[chip], k2.at[chip], k2s.at[0], k2r.at[0], (to, me))

    def k2_group():
        return group(k2.at[pl.ds(0, chips - 1)], k2s.at[0], k2r.at[0])

    for j in range(1, chips):
        start(None, functools.partial(k2_send, j), False)
    tick()

    @scoped
    def k2_wait():
        k2_group().wait_recv()

    k2_wait()
    total = k2[0]
    for j in range(1, chips):
        total = total + k2[j]
    k3[core] = total

    def k3_copy(half):
        return send(k3.at[half], k3.at[half], k3s.at[0], k3r.at[0], (partner, me))

    start(None, functools.partial(k3_copy, core))
    while active:
        tick()
    bias_group().wait_recv()
    total = kb[0]
    for j in range(1, dp_size):
        total = total + kb[j]
    gb_ref[...] = total
    k3_copy(1 - core).wait_recv()
    for half in range(2):
        gk_ref[:, pl.ds(half * (width // 2), width // 2)] = k3[half, :KW]
    for w in range(parts):
        ring_end(w)

    @scoped
    def drain():
        for m in range(n):

            @pl.when(me == m)
            def _(m=m):
                for k in range(parts):
                    for d in ways:
                        count = sent_of(m, k, d)
                        if count:
                            ref = gathers[k].at[pl.ds(0, count * tokens)]
                            group(ref, us.at[k, d], ur.at[k, 0]).wait_send()

        for w in range(parts):
            group(finals[w].at[:, :, pl.ds(0, chips - 1)], rs.at[w], rr.at[w, 0]).wait_send()
            group(finals[w].at[1 - core], ds.at[w], dr.at[w]).wait_send()
        for r in range(sum_parts):
            ref = sums[r].at[pl.ds(0, (n - 1) * tokens)]
            group(ref, zs.at[r], zr.at[r, 0]).wait_send()
        bias_group().wait_send()
        k1_group().wait_send()
        k2_group().wait_send()
        for cond, make in pending:
            if cond is None:
                make().wait_send()
            else:

                @pl.when(cond)
                def _(make=make):
                    make().wait_send()

    drain()


def shards(n, dp_size, inputs, saved_hidden, upstream, w_in, w_out, kernel):
    chips = dp_size // 2
    tokens, width = inputs.shape[1:]
    hidden = w_in.shape[1]
    total_rows = n * tokens
    up_wide = cuts(width, 256, UP_SHARES)
    mix_wide = cuts(width, 64 * chips, MIX_SHARES)
    sum_wide = cuts(width, 256, SUM_SHARES)
    up_parts, mix_parts, sum_parts = len(up_wide), len(mix_wide), len(sum_wide)
    parts = up_parts + mix_parts
    rows_out = -(-hidden // (4 * chips * 8)) * 8
    high = rows_out * 4 * chips
    rows_of = [rows_out] * up_parts + [wide // (4 * chips) for wide in mix_wide]
    sizes = [(rows_out, wide) for wide in up_wide] + [
        (rows, hidden) for rows in rows_of[up_parts:]
    ]
    dma = pltpu.SemaphoreType.DMA
    bits = chips.bit_length() - 1
    vmem = pl.BlockSpec(memory_space=pltpu.VMEM)
    hbm = pl.BlockSpec(memory_space=pltpu.HBM)
    shape = jax.ShapeDtypeStruct
    grad_inputs, grad_kernel, grad_bias, *finals = pl.pallas_call(
        functools.partial(body, n, dp_size, up_wide, mix_wide, sum_wide, rows_of),
        out_shape=[shape((tokens, width), BF16), shape((KW, width), F32), shape((1, hidden), F32)]
        + [shape((2, 2, chips) + size, BF16) for size in sizes],
        in_specs=[hbm] * 5 + [vmem],
        out_specs=[vmem] * (3 + parts),
        scratch_shapes=[pltpu.VMEM((2 * chips * r, c), F32) for r, c in sizes]
        + [pltpu.VMEM((2 * chips * r, c), BF16) for r, c in sizes] * 2
        + [pltpu.VMEM((2, chips - 1) + size, BF16) for size in sizes] * 2
        + [pltpu.VMEM((total_rows, wide), BF16) for wide in up_wide + mix_wide]
        + [pltpu.VMEM((total_rows, wide), BF16) for wide in sum_wide]
        + [pltpu.VMEM((n + 1, tokens, wide), BF16) for wide in sum_wide]
        + [
            pltpu.VMEM((total_rows, hidden), BF16),
            pltpu.VMEM((width, hidden), BF16),
            pltpu.VMEM((hidden, width), BF16),
            pltpu.VMEM((total_rows, high), BF16),
            pltpu.VMEM((total_rows, hidden), BF16),
            pltpu.VMEM((tokens + 2 * EDGE, width), BF16),
            pltpu.VMEM((tokens + 2 * EDGE, width), BF16),
            pltpu.VMEM((1, hidden), F32),
            pltpu.VMEM((dp_size, 1, hidden), F32),
            pltpu.VMEM((3, 8, width // 2), F32),
            pltpu.VMEM((n, 8, width // 2), F32),
            pltpu.VMEM((chips, 8, width // 2), F32),
            pltpu.VMEM((2, 8, width // 2), F32),
            dma((3,)), dma((n,)), dma((up_parts,)),
            dma((2,)), dma((2,)),
            dma((parts, 2)), dma((parts, n)),
            dma((sum_parts,)), dma((sum_parts, n + 1)),
            dma((parts,)), dma((parts,)),
            dma((parts,)), dma((parts, 2 * bits)),
            dma((parts,)), dma((parts,)),
            dma((sum_parts, 2)), dma((sum_parts, 2)),
            dma((1,)), dma((1,)),
            dma((1,)), dma((1,)),
            dma((1,)), dma((1,)),
            dma((1,)), dma((1,)),
            dma((1,)), dma((1,)),
        ],
        compiler_params=pltpu.CompilerParams(
            collective_id=0, has_side_effects=True, vmem_limit_bytes=VMEM if total_rows <= ROWS else 67043328
        ),
    )(
        inputs[0],
        saved_hidden[0],
        upstream[0],
        w_in,
        w_out,
        kernel,
    )
    outs = [f.reshape(high, wide) for f, wide in zip(finals, up_wide)]
    outs += [f.reshape(wide, hidden) for f, wide in zip(finals[up_parts:], mix_wide)]
    return tuple(
        pl.pallas_call(
            functools.partial(widen, up_wide, mix_wide),
            out_shape=[
                shape((1, tokens, width), BF16),
                shape((width, hidden), F32),
                shape((hidden, width), F32),
                shape((hidden,), F32),
                shape((KW, width), F32),
            ],
            in_specs=[vmem] * (parts + 3),
            out_specs=[hbm] * 3 + [vmem] + [hbm],
            scratch_shapes=[pltpu.VMEM((wide, hidden), F32) for wide in mix_wide]
            + [pltpu.VMEM((hidden, wide), F32) for wide in up_wide]
            + [dma((parts + 2,))],
            compiler_params=pltpu.CompilerParams(vmem_limit_bytes=24 * 2**20),
        )(*outs, grad_inputs, grad_kernel, grad_bias)
    )


def widen(up_wide, mix_wide, *refs):
    up_parts, mix_parts = len(up_wide), len(mix_wide)
    parts = up_parts + mix_parts
    finals, (gin, gk, gb), refs = refs[:parts], refs[parts : parts + 3], refs[parts + 3 :]
    gin_out, rows_out, cols_out, gb_out, gk_out, *refs = refs
    rows, cols, sem = refs[:mix_parts], refs[mix_parts:-1], refs[-1]
    copies = [
        pltpu.make_async_copy(gin, gin_out.at[0], sem.at[parts]),
        pltpu.make_async_copy(gk, gk_out, sem.at[parts + 1]),
    ]
    for copy in copies:
        copy.start()
    gb_out[...] = gb[0]

    def widen_one(source, target):
        high = target.shape[0]
        step = 128

        def widen_step(i, _):
            at = pl.ds(pl.multiple_of(i * step, step), step)
            target[at, :] = source[at, :].astype(F32)
            return 0

        lax.fori_loop(0, high // step, widen_step, 0)

    for c in range(mix_parts):
        widen_one(finals[up_parts + c], rows[c])
        at = pl.ds(sum(mix_wide[:c]), mix_wide[c])
        copies.append(pltpu.make_async_copy(rows[c], rows_out.at[at], sem.at[c]))
        copies[-1].start()
    for c in range(up_parts):
        widen_one(finals[c], cols[c])
        at = pl.ds(sum(up_wide[:c]), up_wide[c])
        copies.append(pltpu.make_async_copy(cols[c], cols_out.at[:, at], sem.at[mix_parts + c]))
        copies[-1].start()
    for copy in copies:
        copy.wait()


def solution(mesh):
    in_specs = (
        P("dp", "tp", None),
        P("dp", None, "tp"),
        P("dp", "tp", None),
        P(None, "tp"),
        P("tp", None),
        P(),
    )
    out_specs = (P("dp", "tp", None), P(None, "tp"), P("tp", None), P("tp"), P())
    return jax.shard_map(
        functools.partial(shards, mesh.shape["tp"], mesh.shape["dp"]),
        mesh=mesh,
        in_specs=in_specs,
        out_specs=out_specs,
        check_vma=False,
    )
```
